32 devices in a mesh: rep: 2 (over y), tile: 4 (over z), pen: 2 (over x), sub: 2 (over core).
Axes of the slice: x: 2, y: 2, z: 4, core: 2. Of those that a mesh axis runs over, the one named last changes fastest.
Arguments:
- positions: float32 [6, 4, 2, 512], P('rep', 'tile', 'pen'), parts along dimension 0, may hold values from 0 to 256, as said below
- velocities: float32 [6, 4, 2, 512], P('rep', 'tile', 'pen'), parts along dimension 0, may hold values from -5 to 5
- charges: float32 [8, 2, 512], P(('rep', 'tile'), 'pen'), parts along dimension 0, may hold values from -3 to 3
- inverse_mass: float32 [8, 2, 512], P(('rep', 'tile'), 'pen'), parts along dimension 0, may hold values from 0.06 to 1
- export_rows: int32 [8, 2, 128], P(('rep', 'tile'), 'pen'), parts along dimension 0, may hold values from 0 to 511, as said below
- partners: int32 [8, 2, 64, 512], P(('rep', 'tile'), 'pen', 'sub'), parts along dimension 0, may hold values from 0 to 1663, as said below
- bond_partners: int32 [8, 2, 4, 512], P(('rep', 'tile'), 'pen', 'sub'), parts along dimension 0, may hold values from 0 to 511, as said below
- bond_rest: float32 [8, 2, 4, 512], P(('rep', 'tile'), 'pen', 'sub'), parts along dimension 0, may hold values from 1 to 8
- block_offsets: int32 [6, 4, 2, 512], P('rep', 'tile', 'pen'), parts along dimension 0, may hold values from -1 to 254, as said below
Outputs:
- final_positions: float32 [6, 4, 2, 512], P('rep', 'tile', 'pen'), parts along dimension 0
- final_velocities: float32 [6, 4, 2, 512], P('rep', 'tile', 'pen'), parts along dimension 0
- potential: float32 [8, 2, 512], P(('rep', 'tile'), 'pen', 'sub'), parts along dimension 0
The draws below stay inside these ranges and needn't reach their ends.
There are 2 independent parts, one for each index of `rep`. The reference program is written for one: setup_inputs(seed, part) draws one part's arguments, and reference() takes and returns one part's arrays. A program takes and returns all parts, laid end to end along the dimension named above; each array names one. Nothing has to cross between parts.
Inputs may be any that keep to these rules, and one draw needn't show every extreme that they name: `positions`: coordinates of an atom lie strictly between its block offset + 1 and its block offset + 2, coordinate by coordinate. `block_offsets`: for the patch (t, p), x offsets lie in t * 64 - 1 to t * 64 + 62 and y offsets in p * 128 - 1 to p * 128 + 126; z offsets lie in -1 to 254. `export_rows`: rows of the patch's own atoms. `partners`: columns of the patch's table; columns 1024 to 1151 are never named. Slots that an atom does not use name the atom itself. `bond_partners`: rows of the patch's own atoms.
All inputs are finite; a program needn't handle non-finite values.
Results may differ from the reference program's by a relative error of at most 0.0005.
Values sent between devices are 32-bit elements; how exact they have to be, the bound alone decides.
A program may use at most 128 MiB of HBM per device.

```python
import math
import jax
import jax.numpy as jnp
from jax import lax

GRID = 256
ATOMS = 512
NEIGH = 32
BONDS = 2
INNER = 4
EXPORT = 128
N_TILE = 4
N_PEN = 2


def atom_layout(key):
    keys = jax.random.split(jax.random.fold_in(key, 17), 4)
    shape = (N_TILE, N_PEN, ATOMS)
    planes_x = GRID // N_TILE
    rows_y = GRID // N_PEN
    tiles = jnp.arange(N_TILE, dtype=jnp.int32)[:, None, None]
    pens = jnp.arange(N_PEN, dtype=jnp.int32)[None, :, None]
    atoms = jnp.arange(ATOMS, dtype=jnp.int32)[None, None, :]
    offset_x = tiles * planes_x - 1 + jax.random.randint(keys[0], shape, 0, planes_x)
    offset_y = pens * rows_y - 1 + jax.random.randint(keys[1], shape, 0, rows_y)
    offset_z = jnp.clip(atoms * GRID // ATOMS + jax.random.randint(keys[2], shape, -2, 3), -1, GRID - 2)
    offsets = jnp.stack([offset_x, offset_y, jnp.broadcast_to(offset_z, shape)]).astype(jnp.int32)
    return (offsets, keys[3])


def draw_positions(key, part):
    offsets, frac_key = atom_layout(key)
    frac = jnp.clip(0.5 + 0.18 * jax.random.normal(frac_key, offsets.shape, jnp.float32), 0.05, 0.95)
    return offsets.astype(jnp.float32) + 1.0 + frac


def draw_block_offsets(key, part):
    offsets, frac_key = atom_layout(key)
    return offsets


def draw_export_rows(key, part):
    drawn = jax.random.fold_in(key, 23)
    stride = ATOMS // EXPORT
    rows = jnp.arange(EXPORT, dtype=jnp.int32)[None, None, :] * stride
    return (rows + jax.random.randint(drawn, (N_TILE, N_PEN, EXPORT), 0, stride)).astype(jnp.int32)


def draw_partners(key, part):
    keys = jax.random.split(jax.random.fold_in(key, 29), 5)
    shape = (N_TILE, N_PEN, 2 * NEIGH, ATOMS)
    atoms = jnp.arange(ATOMS, dtype=jnp.int32)[None, None, None, :]
    reach = max(1, 6 * ATOMS // GRID)
    near = jnp.clip(atoms + jax.random.randint(keys[0], shape, -reach, reach + 1), 0, ATOMS - 1)
    neighbour = jax.random.randint(keys[1], shape, 0, 8)
    neighbour = jnp.where(neighbour >= 4, neighbour + 1, neighbour)
    spread = max(1, 6 * EXPORT // GRID)
    column = jnp.clip(atoms * EXPORT // ATOMS + jax.random.randint(keys[2], shape, -spread, spread + 1), 0, EXPORT - 1)
    distant = ATOMS + neighbour * EXPORT + column
    picked = jnp.where(jax.random.randint(keys[3], shape, 0, 2) == 0, near, distant)
    live = jax.random.randint(keys[4], (N_TILE, N_PEN, 1, ATOMS), NEIGH // 2, 2 * NEIGH + 1)
    slots = jnp.arange(2 * NEIGH, dtype=jnp.int32)[None, None, :, None]
    return jnp.where(slots < live, picked, atoms).astype(jnp.int32)


def draw_bond_partners(key, part):
    keys = jax.random.split(jax.random.fold_in(key, 31), 2)
    shape = (N_TILE, N_PEN, 2 * BONDS, ATOMS)
    atoms = jnp.arange(ATOMS, dtype=jnp.int32)[None, None, None, :]
    length = jax.random.randint(keys[0], shape, 1, 4)
    upward = jax.random.randint(keys[1], shape, 0, 2) * 2 - 1
    return jnp.clip(atoms + length * upward, 0, ATOMS - 1).astype(jnp.int32)


def block_levels(stream_key, shape, cuts, smallest, largest):
    def one(dim, parts):
        steps = jax.random.uniform(jax.random.fold_in(jax.random.fold_in(stream_key, 6), dim), (parts,), jnp.float32, smallest / len(cuts), largest / len(cuts))
        return jnp.repeat(jnp.exp(steps), shape[dim] // parts).reshape((-1,) + (1,) * (len(shape) - dim - 1))

    loudness = one(*cuts[0])
    for cut in cuts[1:]:
        loudness = loudness * one(*cut)
    return loudness


def normal_values(stream_key, shape, width, limit, shards=(), kind=jnp.bfloat16):
    factor_of = block_levels(stream_key, shape, shards, -0.22, 0.18) if shards else 1.0
    entries = jax.random.normal(stream_key, shape, jnp.float32) * width * factor_of
    return jnp.minimum(jnp.maximum(entries, -limit), limit).astype(kind)


def setup_inputs(seed: int = 0, part: int = 0) -> dict:
    seeds = jax.random.split(jax.random.key(seed), 10)
    part_keys = jax.random.split(jax.random.fold_in(seeds[9], part), 10)
    return {
        "positions": draw_positions(jax.random.fold_in(jax.random.fold_in(seeds[9], part), 71), part),
        "velocities": normal_values(part_keys[1], (3, N_TILE, N_PEN, ATOMS), 1.0, 5.0, ((1, 4), (2, 2)), jnp.float32),
        "charges": normal_values(part_keys[2], (N_TILE, N_PEN, ATOMS), 0.5, 3.0, ((0, 4), (1, 2)), jnp.float32),
        "inverse_mass": jnp.clip(jnp.exp(math.log(1.0) - 2.8134107 * jax.random.uniform(part_keys[3], (N_TILE, N_PEN, ATOMS), jnp.float32) ** block_levels(part_keys[3], (N_TILE, N_PEN, ATOMS), ((0, 4), (1, 2)), -0.2, 0.2)), 0.06, 1.0),
        "export_rows": draw_export_rows(jax.random.fold_in(jax.random.fold_in(seeds[9], part), 71), part),
        "partners": draw_partners(jax.random.fold_in(jax.random.fold_in(seeds[9], part), 71), part),
        "bond_partners": draw_bond_partners(jax.random.fold_in(jax.random.fold_in(seeds[9], part), 71), part),
        "bond_rest": jnp.clip(1.0 + 7.0 * jax.random.uniform(part_keys[7], (N_TILE, N_PEN, 2 * BONDS, ATOMS), jnp.float32) ** block_levels(part_keys[7], (N_TILE, N_PEN, 2 * BONDS, ATOMS), ((0, 4), (1, 2), (2, 2)), -0.2, 0.2), 1.0, 8.0),
        "block_offsets": draw_block_offsets(jax.random.fold_in(jax.random.fold_in(seeds[9], part), 71), part),
    }


time_step = 0.1
coulomb = 30.0
bond_stiffness = 0.2
soften = 1.0
cutoff_sq = 144.0
ewald_beta = 0.32
highest = lax.Precision.HIGHEST

def spline_pieces(frac):
    rest = 1.0 - frac
    cube = frac * frac * frac
    square = frac * frac
    return (rest * rest * rest / 6.0, (3.0 * cube - 6.0 * square + 4.0) / 6.0, (-3.0 * cube + 3.0 * square + 3.0 * frac + 1.0) / 6.0, cube / 6.0)

def axis_weights(cells, offset, frac, wrapped):
    place = cells[:, None] - offset[None, :]
    if wrapped:
        place = jnp.mod(place, GRID)
    pieces = spline_pieces(frac)
    total = jnp.zeros(place.shape, frac.dtype)
    for order in range(4):
        total = total + jnp.where(place == order, pieces[order][None, :], 0.0)
    return total

def patch_weights(place, offsets, tile_index, pen_index, planes_x, rows_y):
    frac = place - (offsets.astype(place.dtype) + 1.0)
    cells_x = tile_index * planes_x - 1 + jnp.arange(planes_x + 3, dtype=jnp.int32)
    cells_y = pen_index * rows_y - 1 + jnp.arange(rows_y + 3, dtype=jnp.int32)
    weight_x = axis_weights(cells_x, offsets[0], frac[0], False)
    weight_y = axis_weights(cells_y, offsets[1], frac[1], False)
    depth = axis_weights(jnp.arange(GRID, dtype=jnp.int32), offsets[2], frac[2], True)
    plane = (weight_x[:, None, :] * weight_y[None, :, :]).reshape(-1, place.shape[1])
    return (plane, depth)

def influence(freq_x, freq_y, freq_z):

    def signed(freq):
        return jnp.where(freq > GRID // 2, freq - GRID, freq).astype(jnp.float32)

    def modulus(freq):
        angle = 2.0 * math.pi / GRID * freq.astype(jnp.float32)
        real = (1.0 + 4.0 * jnp.cos(angle) + jnp.cos(2.0 * angle)) / 6.0
        imag = (4.0 * jnp.sin(angle) + jnp.sin(2.0 * angle)) / 6.0
        return 1.0 / (real * real + imag * imag)
    sx, sy, sz = (signed(freq_x), signed(freq_y), signed(freq_z))
    m_sq = (sx[:, None, None] ** 2 + sy[None, :, None] ** 2 + sz[None, None, :] ** 2) / float(GRID * GRID)
    anchor = (freq_x[:, None, None] == 0) & (freq_y[None, :, None] == 0) & (freq_z[None, None, :] == 0)
    safe = jnp.where(anchor, 1.0, m_sq)
    value = jnp.exp(-(math.pi / ewald_beta) ** 2 * safe) / (math.pi * float(GRID) ** 3 * safe)
    value = value * modulus(freq_x)[:, None, None] * modulus(freq_y)[None, :, None] * modulus(freq_z)[None, None, :]
    return jnp.where(anchor, 0.0, value)

def hartley(field, axis):
    spectrum = jnp.fft.fft(field, axis=axis)
    return jnp.real(spectrum) - jnp.imag(spectrum)

def pair_force(table, own, charge, neighbours, bonded, rest):
    near = table[:, neighbours]
    delta = own[:, None, :] - near[:3]
    dist_sq = lax.optimization_barrier(jnp.sum(delta * delta, axis=0))
    taper = jnp.where(dist_sq < cutoff_sq, (1.0 - dist_sq / cutoff_sq) ** 2, 0.0)
    strength = coulomb * charge[None, :] * near[3] * taper * (dist_sq + soften) ** (-1.5)
    force = lax.optimization_barrier(jnp.sum(strength[None] * delta, axis=1))
    bond_delta = own[:, None, :] - table[:3][:, bonded]
    length = jnp.sqrt(lax.optimization_barrier(jnp.sum(bond_delta * bond_delta, axis=0)) + soften)
    pull = -bond_stiffness * (length - rest) / length
    return force + lax.optimization_barrier(jnp.sum(pull[None] * bond_delta, axis=1))

def halo_table(coords, charges, export_rows, tiles, pens):
    index = jnp.broadcast_to(export_rows[None], (3,) + export_rows.shape)
    sent = jnp.take_along_axis(coords, index, axis=3)
    sent_charge = jnp.take_along_axis(charges, export_rows, axis=2)
    stacked = jnp.concatenate([sent, sent_charge[None]], axis=0)
    blocks = []
    for across in range(3):
        near_x = tiles + across - 1
        move_x = jnp.where(near_x < 0, -float(GRID), jnp.where(near_x >= N_TILE, float(GRID), 0.0))
        for along in range(3):
            near_y = pens + along - 1
            move_y = jnp.where(near_y < 0, -float(GRID), jnp.where(near_y >= N_PEN, float(GRID), 0.0))
            moved = jnp.roll(stacked, (1 - across, 1 - along), axis=(1, 2))
            blank = jnp.zeros((N_TILE, N_PEN), jnp.float32)
            offset = jnp.stack([jnp.broadcast_to(move_x[:, None], (N_TILE, N_PEN)), jnp.broadcast_to(move_y[None, :], (N_TILE, N_PEN)), blank, blank])
            blocks.append(moved + offset[..., None].astype(moved.dtype))
    own = jnp.concatenate([coords, charges[None]], axis=0)
    return jnp.concatenate([own] + blocks, axis=3)

def reference(positions, velocities, charges, inverse_mass, export_rows, partners, bond_partners, bond_rest, block_offsets):
    planes_x = GRID // N_TILE
    rows_y = GRID // N_PEN
    patch_count = N_TILE * N_PEN
    tiles = jnp.arange(N_TILE, dtype=jnp.int32)
    pens = jnp.arange(N_PEN, dtype=jnp.int32)
    tile_ids = jnp.repeat(tiles, N_PEN)
    pen_ids = jnp.tile(pens, N_TILE)
    flat_partners = partners.reshape(patch_count, -1, ATOMS)
    flat_bonds = bond_partners.reshape(patch_count, -1, ATOMS)
    flat_rest = bond_rest.reshape(patch_count, -1, ATOMS)
    flat_charge = charges.reshape(patch_count, ATOMS)
    coords, speeds = (positions, velocities)

    def patch_force(item):
        table, own, charge, neighbours, bonded, rest = item
        return pair_force(table, own, charge, neighbours, bonded, rest)
    for step in range(INNER):
        table = halo_table(coords, charges, export_rows, tiles, pens)
        flat_table = jnp.transpose(table, (1, 2, 0, 3)).reshape(patch_count, 4, -1)
        flat_coords = jnp.transpose(coords, (1, 2, 0, 3)).reshape(patch_count, 3, ATOMS)
        force = lax.map(patch_force, (flat_table, flat_coords, flat_charge, flat_partners, flat_bonds, flat_rest))
        force = jnp.transpose(force.reshape(N_TILE, N_PEN, 3, ATOMS), (2, 0, 1, 3))
        speeds = speeds + time_step * inverse_mass[None] * force
        coords = coords + time_step * speeds
    flat_coords = jnp.transpose(coords, (1, 2, 0, 3)).reshape(patch_count, 3, ATOMS)
    flat_offsets = jnp.transpose(block_offsets, (1, 2, 0, 3)).reshape(patch_count, 3, ATOMS)

    def spread_patch(item):
        place, offsets, charge, tile_index, pen_index = item
        plane, depth = patch_weights(place, offsets, tile_index, pen_index, planes_x, rows_y)
        local = jnp.einsum('pa,za->pz', plane * charge[None, :], depth, precision=highest)
        return local.reshape(planes_x + 3, rows_y + 3, GRID)
    blocks = lax.map(spread_patch, (flat_coords, flat_offsets, flat_charge, tile_ids, pen_ids))
    blocks = blocks.reshape(N_TILE, N_PEN, planes_x + 3, rows_y + 3, GRID)
    inner_x = blocks[:, :, 1:planes_x + 1]
    from_above = jnp.roll(blocks[:, :, 0:1], -1, axis=0)
    from_below = jnp.roll(blocks[:, :, planes_x + 1:], 1, axis=0)
    inner_x = inner_x.at[:, :, 0:2].add(from_below).at[:, :, planes_x - 1:].add(from_above)
    from_right = jnp.roll(inner_x[:, :, :, 0:1], -1, axis=1)
    from_left = jnp.roll(inner_x[:, :, :, rows_y + 1:], 1, axis=1)
    core = inner_x[:, :, :, 1:rows_y + 1]
    core = core.at[:, :, :, 0:2].add(from_left).at[:, :, :, rows_y - 1:].add(from_right)
    charge_grid = jnp.transpose(core, (0, 2, 1, 3, 4)).reshape(GRID, GRID, GRID)
    spectrum = hartley(hartley(hartley(charge_grid, 2), 1), 0)
    freq = jnp.arange(GRID, dtype=jnp.int32)
    weighted = spectrum * influence(freq, freq, freq)
    potential_grid = hartley(hartley(hartley(weighted, 0), 1), 2)
    padded = jnp.pad(potential_grid, ((1, 2), (1, 2), (0, 0)), mode='wrap')

    def read_patch(item):
        place, offsets, tile_index, pen_index = item
        plane, depth = patch_weights(place, offsets, tile_index, pen_index, planes_x, rows_y)
        corner = (tile_index * planes_x, pen_index * rows_y, jnp.int32(0))
        block = lax.dynamic_slice(padded, corner, (planes_x + 3, rows_y + 3, GRID))
        values = jnp.dot(block.reshape(-1, GRID), depth, precision=highest)
        return lax.optimization_barrier(jnp.sum(values * plane, axis=0))
    potential = lax.map(read_patch, (flat_coords, flat_offsets, tile_ids, pen_ids))
    return (coords, speeds, potential.reshape(N_TILE, N_PEN, ATOMS))
```

```python
import functools
import math

import jax
import jax.numpy as jnp
import numpy as np
from jax import lax
from jax.experimental import pallas as pl
from jax.experimental.pallas import tpu as pltpu
from jax.sharding import PartitionSpec as P

GRID = 256
INNER = 4
LANES = 128
LOW = 128

time_step = 0.1
coulomb = 30.0
bond_stiffness = 0.2
soften = 1.0
cutoff_sq = 144.0
ewald_beta = 0.32

f32 = jnp.float32
bf16 = jnp.bfloat16


def lane_gather(rows, low):
    return jnp.take_along_axis(rows, low, axis=1, mode="promise_in_bounds")


def split(value):
    high = value.astype(bf16)
    return high, (value - high.astype(f32)).astype(bf16)


def single(left, right, turned=False):
    dims = (((1,), (1 if turned else 0,)), ((), ()))
    return lax.dot_general(left, right, dims, preferred_element_type=f32)


def product(left, right, turned=False):
    return single(left[0], right[0], turned) + (
        single(left[0], right[1], turned) + single(left[1], right[0], turned)
    )


def half_product(left, right, turned=False):
    return single(left[0], right, turned) + single(left[1], right, turned)


def spline(place, frac):
    rest = 1.0 - frac
    square = frac * frac
    cube = square * frac
    pieces = (
        rest * rest * rest / 6.0,
        (3.0 * cube - 6.0 * square + 4.0) / 6.0,
        (-3.0 * cube + 3.0 * square + 3.0 * frac + 1.0) / 6.0,
        cube / 6.0,
    )
    total = jnp.zeros(place.shape, f32)
    for order in range(4):
        total = jnp.where(place == order, pieces[order], total)
    return total


def wide_row(row):
    return jnp.broadcast_to(row, (8, LANES))


def stacked(rows):
    place = lax.broadcasted_iota(jnp.int32, (8, LANES), 0)
    total = jnp.zeros((8, LANES), rows[0].dtype)
    for r, row in enumerate(rows):
        total = jnp.where(place == r, wide_row(row), total)
    return total


def program_kernel(
    lines_ref, squares_ref,
    pos_hbm, vel_hbm, chg_hbm, imass_hbm, shown_hbm, parts_hbm, bonds_hbm, rest_hbm, offs_hbm,
    mine_hbm, cas_hbm, wide_hbm, tall_hbm, along_hbm, across_hbm,
    pos_out, vel_out, pot_out,
    pos_in, vel_in, chg_in, imass_in, shown_in, parts_in, bonds_in, rest_in, offs_in,
    mine_ref, cas_ref, wide_ref, tall_ref, along_ref, across_ref,
    parts_all, bonds_all, rest_all,
    mine, sent, beside, half_sent, half_recv, static_all, pos_all, vel_sent, vel_far,
    low_ref, blk_ref, shx_ref, shy_ref, qq_ref, near_ref, bforce, bidx_ref, brest_ref,
    grid, wx, wy, wyq, wz, part_sent, part_recv, pos_fin, vel_fin, pot_fin,
    load_sem, out_sem, step_send, step_recv, half_send_sem, half_recv_sem,
    pair_send, pair_recv, static_send, static_recv, place_send, place_recv, part_send_sem, part_recv_sem,
    *, tiles, pens, subs, planes, deep, share, lows, chunk, keep,
):
    ti, pi, si = lax.axis_index("tile"), lax.axis_index("pen"), lax.axis_index("sub")
    local = pens * subs
    group = tiles * local
    me = (ti * pens + pi) * subs + si
    atoms = pos_in.shape[3]
    width = atoms // subs
    chunks = width // LANES
    own_blocks = atoms // LANES
    slots = parts_all.shape[1]
    groups = subs * slots // 8
    bond_rows = bonds_all.shape[1]

    offsets = []
    for i in range(3):
        for j in range(3):
            step = ((i - 1) % tiles, (j - 1) % pens)
            if step != (0, 0) and step not in offsets:
                offsets.append(step)

    def remote(src, dst, send, recv, device):
        return pltpu.make_async_remote_copy(
            src_ref=src, dst_ref=dst, send_sem=send, recv_sem=recv,
            device_id=device, device_id_type=pl.DeviceIdType.MESH,
        )

    def tile_at(s):
        if tiles & (tiles - 1):
            return lax.rem(ti + s, tiles)
        total, bit = 0, 1
        while bit < tiles:
            total = total + lax.rem(lax.rem(lax.div(ti, bit), 2) + lax.rem(lax.div(s, bit), 2), 2) * bit
            bit *= 2
        return total

    def peer(d):
        s, rest = lax.div(d, local), lax.rem(d, local)
        t = tile_at(s)
        p = lax.rem(pi + lax.div(rest, subs), pens)
        q = lax.rem(si + lax.rem(rest, subs), subs)
        return {"tile": t, "pen": p, "sub": q}, (t * pens + p) * subs + q

    def each_peer(body):
        def step(d, carry):
            body(d, *peer(d))
            return carry

        lax.fori_loop(1, group, step, 0)

    half_lanes = pl.ds(pl.multiple_of(si * width, LANES), width)
    first_loads = [
        (parts_hbm.at[0, 0, :, half_lanes], parts_all.at[si]),
        (bonds_hbm.at[0, 0, :, half_lanes], bonds_all.at[si]),
        (rest_hbm.at[0, 0, :, half_lanes], rest_all.at[si]),
        (parts_hbm, parts_in), (bonds_hbm, bonds_in), (rest_hbm, rest_in),
        (pos_hbm, pos_in), (vel_hbm, vel_in), (chg_hbm, chg_in), (imass_hbm, imass_in),
        (shown_hbm, shown_in), (offs_hbm, offs_in),
    ]
    later_loads = [
        (mine_hbm.at[:, me], mine_ref), (cas_hbm, cas_ref), (wide_hbm, wide_ref), (tall_hbm, tall_ref),
        (along_hbm, along_ref), (across_hbm, across_ref),
    ]
    loads = [
        pltpu.make_async_copy(src, dst, load_sem.at[k]) for k, (src, dst) in enumerate(first_loads + later_loads)
    ]
    for copy in loads:
        copy.start()

    barrier = pltpu.get_barrier_semaphore()

    def greet(d, device, g):
        pl.semaphore_signal(barrier, inc=1, device_id=device, device_id_type=pl.DeviceIdType.MESH)

    each_peer(greet)
    for copy in loads[: len(first_loads)]:
        copy.wait()

    for c in range(chunks):
        lanes = pl.ds(pl.multiple_of(si * width + c * LANES, LANES), LANES)
        rows = [pos_in[r, 0, :, lanes] for r in range(3)] + [chg_in[0, :, lanes]]
        rows += [vel_in[r, 0, :, lanes] for r in range(3)] + [imass_in[0, :, lanes]]
        mine[c] = stacked(rows)
        offset = stacked([offs_in[r, 0, :, lanes].astype(f32) for r in range(3)])
        static_all[me, :, c * LANES : (c + 1) * LANES] = offset[:4]
    for step in range(1, subs):
        other = lax.rem(si + step, subs)
        for c in range(chunks):
            lanes = pl.ds(pl.multiple_of(other * width + c * LANES, LANES), LANES)
            half_recv[0, other, c] = stacked([pos_in[r, 0, :, lanes] for r in range(3)] + [chg_in[0, :, lanes]])[:4]

    shown = jnp.broadcast_to(shown_in[0], (8, LANES))
    shown_low, shown_high = shown & (LANES - 1), shown >> 7

    def step_copy(n, slot, q):
        dt, dp = offsets[slot]
        back = offsets.index(((-dt) % tiles, (-dp) % pens))
        device = {"tile": lax.rem(ti + dt, tiles), "pen": lax.rem(pi + dp, pens), "sub": q}
        return remote(sent.at[n], beside.at[n, back, si], step_send.at[n, slot, q], step_recv.at[n, back, si], device)

    def half_copy(n, step):
        other = lax.rem(si + step, subs)
        return remote(
            half_sent.at[n], half_recv.at[n, si], half_send_sem.at[n, step], half_recv_sem.at[n, si], {"sub": other}
        )

    def show(n):
        total = jnp.zeros((8, LANES), f32)
        for c in range(chunks):
            total = jnp.where(shown_high == si * chunks + c, lane_gather(mine[c], shown_low), total)
        sent[n] = total[:4]

    def send_shown(n):
        for slot in reversed(range(len(offsets))):
            for q in range(subs):
                step_copy(n, slot, q).start()

    def wait_shown(n):
        for slot in range(len(offsets)):
            for q in range(subs):
                remote(
                    sent.at[n], beside.at[n, slot, q], step_send.at[n, slot, q], step_recv.at[n, slot, q], {"sub": si}
                ).wait_recv()
                step_copy(n, slot, q).wait_send()

    show(0)
    pl.semaphore_wait(barrier, group - 1)
    send_shown(0)
    pairs = []
    for step in range(1, subs):
        other = lax.rem(si + step, subs)
        lanes = pl.ds(pl.multiple_of(other * width, LANES), width)
        for k, (source, target) in enumerate(
            ((parts_in, parts_all), (bonds_in, bonds_all), (rest_in, rest_all))
        ):
            pairs.append((k, step, source.at[0, 0, :, lanes], target, other))
    for k, step, source, target, other in pairs:
        remote(source, target.at[si], pair_send.at[k, step], pair_recv.at[k, si], {"sub": other}).start()

    def static_copy(d, device):
        return remote(static_all.at[me], static_all.at[me], static_send.at[d], static_recv.at[me], device)

    each_peer(lambda d, device, g: static_copy(d, device).start())
    for k, step, source, target, other in pairs:
        remote(source, target.at[other], pair_send.at[k, step], pair_recv.at[k, other], {"sub": other}).wait_recv()
        remote(source, target.at[si], pair_send.at[k, step], pair_recv.at[k, si], {"sub": other}).wait_send()

    moves_x, moves_y = [], []
    for i in range(3):
        near = ti + (i - 1)
        moves_x.append(jnp.where(near < 0, -float(GRID), jnp.where(near >= tiles, float(GRID), 0.0)))
        near = pi + (i - 1)
        moves_y.append(jnp.where(near < 0, -float(GRID), jnp.where(near >= pens, float(GRID), 0.0)))
    for c in range(chunks):
        for g in range(groups):
            q, row = divmod(g * 8, slots)
            index = parts_all[q, row : row + 8, c * LANES : (c + 1) * LANES]
            high = index >> 7
            block = high
            shx = jnp.zeros((8, LANES), f32)
            shy = jnp.zeros((8, LANES), f32)
            for i in range(3):
                for j in range(3):
                    if (i, j) == (1, 1):
                        continue
                    hit = high == own_blocks + i * 3 + j
                    step = ((i - 1) % tiles, (j - 1) % pens)
                    block = jnp.where(hit, own_blocks + offsets.index(step), block)
                    if i != 1:
                        shx = jnp.where(hit, moves_x[i], shx)
                    if j != 1:
                        shy = jnp.where(hit, moves_y[j], shy)
            low_ref[c, g] = index & (LANES - 1)
            blk_ref[c, g] = block
            shx_ref[c, g] = shx
            shy_ref[c, g] = shy
        atom = lax.broadcasted_iota(jnp.int32, (1, LANES), 1) + (si * width + c * LANES)
        every = [(q, b) for q in range(subs) for b in range(bond_rows)]
        for v in range(bidx_ref.shape[1]):
            part = every[v * 8 : v * 8 + 8]
            lanes = slice(c * LANES, (c + 1) * LANES)
            rows = [bonds_all[q, b : b + 1, lanes] for q, b in part]
            rows += [atom] * (8 - len(part))
            bidx_ref[c, v] = stacked(rows)
            brest_ref[c, v] = stacked([rest_all[q, b : b + 1, lanes] for q, b in part])

    def own_tables(rows):
        out = []
        for c in range(chunks):
            out.append((si * chunks + c, [wide_row(mine[c, r : r + 1, :]) for r in rows]))
        return out

    def far_tables(n, rows):
        out = []
        for step in range(1, subs):
            other = lax.rem(si + step, subs)
            for c in range(chunks):
                out.append((other * chunks + c, [wide_row(half_recv[n, other, c, r : r + 1, :]) for r in rows]))
        return out

    def around_tables(n, rows):
        out = []
        for slot in range(len(offsets)):
            patch = beside[n, slot, 0]
            for q in range(1, subs):
                patch = patch + beside[n, slot, q]
            out.append((own_blocks + slot, [wide_row(patch[r : r + 1, :]) for r in rows]))
        return out

    def pick(found, low, block, table):
        for number, sources in table:
            hit = block == number
            found = [jnp.where(hit, lane_gather(source, low), f) for source, f in zip(sources, found)]
        return found

    xyz = (0, 1, 2)

    def near_part(n, wait):
        table = own_tables(xyz)
        for c in range(chunks):
            for g in range(groups):
                found = pick([jnp.zeros((8, LANES), f32)] * 3, low_ref[c, g], blk_ref[c, g], table)
                for r in xyz:
                    near_ref[c, g, r] = found[r]
        if wait:
            for step in range(1, subs):
                other = lax.rem(si + step, subs)
                remote(
                    half_sent.at[n], half_recv.at[n, other], half_send_sem.at[n, step], half_recv_sem.at[n, other],
                    {"sub": other},
                ).wait_recv()
                half_copy(n, step).wait_send()
        more = far_tables(n, xyz)
        for c in range(chunks):
            for g in range(groups):
                found = [near_ref[c, g, r] for r in xyz]
                found = pick(found, low_ref[c, g], blk_ref[c, g], more)
                for r in xyz:
                    near_ref[c, g, r] = found[r]
            own = [wide_row(mine[c, r : r + 1, :]) for r in xyz]
            force = [jnp.zeros((8, LANES), f32)] * 3
            for v in range(bidx_ref.shape[1]):
                index = bidx_ref[c, v]
                near = pick([jnp.zeros((8, LANES), f32)] * 3, index & (LANES - 1), index >> 7, table + more)
                delta = [own[r] - near[r] for r in xyz]
                root = lax.rsqrt(delta[0] * delta[0] + delta[1] * delta[1] + delta[2] * delta[2] + soften)
                pull = -bond_stiffness * (1.0 - brest_ref[c, v] * root)
                force = [force[r] + pull * delta[r] for r in xyz]
            for r in xyz:
                bforce[c, r] = force[r]

    def far_part(n):
        table = around_tables(n, xyz)
        for c in range(chunks):
            own = [wide_row(mine[c, r : r + 1, :]) for r in xyz]
            force = [bforce[c, r] for r in xyz]
            for g in range(groups):
                near = pick([near_ref[c, g, r] for r in xyz], low_ref[c, g], blk_ref[c, g], table)
                delta = [own[0] - (near[0] + shx_ref[c, g]), own[1] - (near[1] + shy_ref[c, g]), own[2] - near[2]]
                dist_sq = delta[0] * delta[0] + delta[1] * delta[1] + delta[2] * delta[2]
                taper = 1.0 - dist_sq * (1.0 / cutoff_sq)
                taper = jnp.where(dist_sq < cutoff_sq, taper * taper, 0.0)
                root = lax.rsqrt(dist_sq + soften)
                strength = qq_ref[c, g] * taper * (root * root * root)
                force = [force[r] + strength * delta[r] for r in xyz]
            scale = mine[c, 7:8, :]
            for r in xyz:
                total = jnp.sum(force[r], axis=0, keepdims=True)
                speed = mine[c, 4 + r : 5 + r, :] + time_step * scale * total
                mine[c, 4 + r : 5 + r, :] = speed
                mine[c, r : r + 1, :] = mine[c, r : r + 1, :] + time_step * speed

    near_part(0, False)
    wait_shown(0)
    table = own_tables((3,)) + far_tables(0, (3,)) + around_tables(0, (3,))
    for c in range(chunks):
        own = wide_row(mine[c, 3:4, :])
        for g in range(groups):
            (near,) = pick([jnp.zeros((8, LANES), f32)], low_ref[c, g], blk_ref[c, g], table)
            qq_ref[c, g] = coulomb * own * near

    def inner(n, carry):
        far_part(n)
        for c in range(chunks):
            half_sent[n + 1, c] = mine[c][:4]
        show(n + 1)
        for step in range(1, subs):
            half_copy(n + 1, step).start()
        send_shown(n + 1)
        near_part(n + 1, True)
        wait_shown(n + 1)
        return carry

    lax.fori_loop(0, INNER - 1, inner, 0)
    far_part(INNER - 1)

    for c in range(chunks):
        lanes = slice(c * LANES, (c + 1) * LANES)
        pos_all[me, :, lanes] = mine[c][:4]
        vel_sent[:, lanes] = mine[c][4:]

    def place_copy(d, device):
        return remote(pos_all.at[me], pos_all.at[me], place_send.at[d], place_recv.at[me], device)

    def place_wait(g):
        remote(pos_all.at[me], pos_all.at[g], place_send.at[0], place_recv.at[g], {"sub": si}).wait_recv()

    def speed_copy(step):
        other = lax.rem(si + step, subs)
        return remote(vel_sent, vel_far.at[si], pair_send.at[3, step], pair_recv.at[3, si], {"sub": other})

    each_peer(lambda d, device, g: place_copy(d, device).start())
    for step in range(1, subs):
        speed_copy(step).start()

    for copy in loads[len(first_loads) :]:
        copy.wait()
    each_peer(
        lambda d, device, g: remote(
            static_all.at[me], static_all.at[g], static_send.at[d], static_recv.at[g], {"sub": si}
        ).wait_recv()
    )
    each_peer(lambda d, device, g: static_copy(d, device).wait_send())
    wide_atoms = local * width
    top = tiles * planes

    def cells(offset, count):
        return lax.broadcasted_iota(jnp.int32, (count, wide_atoms), 0) - offset

    def row_of(ref, t, r):
        return jnp.concatenate([ref[t * local + q, r : r + 1, :] for q in range(local)], axis=1)

    def prepare(t, r):
        offset = row_of(static_all, t, r)
        return offset.astype(jnp.int32), row_of(pos_all, t, r) - (offset + 1.0)

    def depth_of(t):
        offset, frac = prepare(t, 2)
        depth = spline(cells(offset, GRID) & (GRID - 1), frac)
        return split(product((cas_ref[0], cas_ref[1]), split(depth)))

    def clear(j, carry):
        for edge in range(tiles + 1):
            grid[j, edge * planes : edge * planes + 8] = jnp.zeros((8, GRID), f32)
        return carry

    lax.fori_loop(0, share, clear, 0)
    parts = [(c, min(c + chunk, lows), True) for c in range(0, lows, chunk)]
    parts += [(c, min(c + chunk, share), False) for c in range(lows, share, chunk)]

    def spread(s, carry):
        t = tile_at(s)

        def arrived(q, inner_carry):
            place_wait(t * local + lax.rem(pi * subs + si + q, local))
            return inner_carry

        @pl.when(s > 0)
        def _():
            place_wait(t * local + pi * subs + si)

        lax.fori_loop(1, local, arrived, 0)
        offset, frac = prepare(t, 0)
        wx[t] = spline(cells(offset - (t * planes - 1), deep), frac)
        offset, frac = prepare(t, 1)
        rows = spline(cells(offset, GRID) & (GRID - 1), frac)
        wy[t] = product((mine_ref[0], mine_ref[1]), split(rows))
        wyq[...] = wy[t] * row_of(pos_all, t, 3)
        depth = depth_of(t)
        if keep:
            wz[t, 0] = depth[0]
            wz[t, 1] = depth[1]
        base = pl.multiple_of(t * planes, 8)
        for start, stop, exact in parts:
            plane = jnp.concatenate([wx[t] * wyq[k : k + 1, :] for k in range(start, stop)], axis=0)
            if exact:
                values = product(split(plane), depth, True)
            else:
                values = half_product(split(plane), depth[0], True)
            values = values.reshape(stop - start, deep, GRID)
            for k in range(start, stop):
                value = values[k - start]
                grid[k, pl.ds(base, 8)] += value[:8]
                if planes > 8:
                    grid[k, pl.ds(pl.multiple_of(base + 8, 8), planes - 8)] = value[8:planes]
                grid[k, pl.ds(pl.multiple_of(base + planes, 8), 8)] += value[planes : planes + 8]
        return carry


    lax.fori_loop(0, tiles, spread, 0)
    for r in range(3):
        for q in range(subs):
            lanes = slice(q * width, (q + 1) * width)
            pos_fin[r, 0, :, lanes] = pos_all[(ti * pens + pi) * subs + q, r : r + 1, :]
    for r in range(3):
        for step in range(1, subs):
            other = lax.rem(si + step, subs)
            if r == 0:
                remote(
                    vel_sent, vel_far.at[other], pair_send.at[3, step], pair_recv.at[3, other], {"sub": other}
                ).wait_recv()
                speed_copy(step).wait_send()
            vel_fin[r, 0, :, pl.ds(pl.multiple_of(other * width, LANES), width)] = vel_far[other, r : r + 1, :]
        vel_fin[r, 0, :, half_lanes] = vel_sent[r : r + 1, :]
    outs = [
        pltpu.make_async_copy(pos_fin, pos_out, out_sem.at[0]),
        pltpu.make_async_copy(vel_fin, vel_out, out_sem.at[1]),
    ]
    for copy in outs:
        copy.start()

    def transform(exact):
        def step(k, carry):
            grid[k, 0:8] += grid[k, top : top + 8]
            line = grid[k, 0:top]
            spectrum = product((wide_ref[0], wide_ref[1]), split(line))
            m_sq = along_ref[...] + squares_ref[me * share + k]
            anchor = m_sq == 0.0
            value = across_ref[...] * lines_ref[me * share + k] / jnp.where(anchor, 1.0, m_sq)
            weighted = spectrum * jnp.where(anchor, 0.0, value)
            if exact:
                back = product((tall_ref[0], tall_ref[1]), split(weighted))
            else:
                back = half_product((tall_ref[0], tall_ref[1]), weighted.astype(bf16))
            grid[k, 0:top] = back
            grid[k, top : top + 8] = back[0:8]
            return carry

        return step

    lax.fori_loop(0, lows, transform(True), 0)
    lax.fori_loop(lows, share, transform(False), 0)

    def part_copy(g, device):
        return remote(part_sent.at[g], part_recv.at[me], part_send_sem.at[g], part_recv_sem.at[me], device)

    def device_of(g):
        return {"tile": lax.div(g, local), "pen": lax.rem(lax.div(g, subs), pens), "sub": lax.rem(g, subs)}

    def read(n, carry):
        s = tiles - 1 - n
        t = tile_at(s)
        if keep:
            depth = (wz[t, 0], wz[t, 1])
        else:
            depth = depth_of(t)
        base = pl.multiple_of(t * planes, 8)
        total = jnp.zeros((planes + 8, wide_atoms), f32)
        for start, stop, exact in parts:
            rows = [grid[k, pl.ds(base, planes + 8)] for k in range(start, stop)]
            line = jnp.concatenate(rows, axis=0)
            if exact:
                values = product(split(line), depth)
            else:
                values = half_product(split(line), depth[0])
            for k in range(start, stop):
                part = values[(k - start) * (planes + 8) : (k - start + 1) * (planes + 8)]
                total = total + part * wy[t, k : k + 1, :]
        result = jnp.sum(total * wx[t, : planes + 8], axis=0, keepdims=True)
        for q in range(local):
            part_sent[t * local + q] = result[:, q * width : (q + 1) * width]

        @pl.when(s > 0)
        def _():
            g = t * local + pi * subs + si
            part_copy(g, device_of(g)).start()

        def give(q, inner_carry):
            g = t * local + lax.rem(pi * subs + si + q, local)
            part_copy(g, device_of(g)).start()
            return inner_carry

        lax.fori_loop(1, local, give, 0)
        return carry

    lax.fori_loop(0, tiles, read, 0)
    part_recv[me] = part_sent[me]
    each_peer(lambda d, device, g: place_copy(d, device).wait_send())
    each_peer(lambda d, device, g: part_copy(g, device).wait_send())
    each_peer(
        lambda d, device, g: remote(
            part_sent.at[me], part_recv.at[g], part_send_sem.at[g], part_recv_sem.at[g], {"sub": si}
        ).wait_recv()
    )
    pot_fin[0] = jnp.sum(part_recv[...], axis=0)
    last = pltpu.make_async_copy(pot_fin, pot_out, out_sem.at[2])
    last.start()
    for copy in outs + [last]:
        copy.wait()


def halves(table):
    table = jnp.asarray(table.astype(np.float32))
    return jnp.stack(split(table))


def tables(group):
    share = GRID // group
    index = np.arange(GRID)
    angle = 2.0 * math.pi / GRID * np.mod(index[:, None] * index[None, :], GRID)
    cas = np.cos(angle) + np.sin(angle)
    wide = cas[:, np.mod(index - 1, GRID)]
    order = np.array([(r + 1) // 2 if r % 2 else (GRID - r // 2) % GRID for r in range(GRID)])
    dealt = order.reshape(share, group).T
    signed = np.where(index > GRID // 2, index - GRID, index).astype(np.float64)
    turn = 2.0 * math.pi / GRID * index
    real = (1.0 + 4.0 * np.cos(turn) + np.cos(2.0 * turn)) / 6.0
    imag = (4.0 * np.sin(turn) + np.sin(2.0 * turn)) / 6.0
    square = signed**2 / float(GRID * GRID)
    line = np.exp(-((math.pi / ewald_beta) ** 2) * square) / (real * real + imag * imag)
    along = square[:, None] + square[None, :]
    across = line[:, None] * line[None, :] / (math.pi * float(GRID) ** 3)
    flat = dealt.reshape(-1)
    return (
        cas, wide, cas[dealt], line[flat].astype(np.float32), square[flat].astype(np.float32),
        along.astype(np.float32), across.astype(np.float32),
    )


def on_device(
    positions, velocities, charges, inverse_mass, export_rows, partners, bond_partners, bond_rest, block_offsets,
):
    tiles, pens, subs = lax.axis_size("tile"), lax.axis_size("pen"), lax.axis_size("sub")
    local = pens * subs
    group = tiles * local
    atoms, exported = positions.shape[3], export_rows.shape[2]
    slots, bond_rows = partners.shape[2], bond_partners.shape[2]
    width = atoms // subs
    chunks = width // LANES
    groups = subs * slots // 8
    planes = GRID // tiles
    share = GRID // group
    lows = min(share, max(1, -(-LOW // group)))
    chunk = math.gcd(share, 4)
    unit = 8 if chunk % 2 == 0 else 16
    deep = -(-(planes + 8) // unit) * unit
    wide_atoms = local * width
    keep = group * width * GRID * 4 <= 16 * 1024 * 1024
    cas, wide, dealt, line, square, along, across = tables(group)
    around = {((i - 1) % tiles, (j - 1) % pens) for i in range(3) for j in range(3)} - {(0, 0)}
    near = len(around)
    bond_tiles = -(-subs * bond_rows // 8)
    assert exported == LANES and slots % 8 == 0 and planes % 8 == 0
    hbm = pl.BlockSpec(memory_space=pltpu.HBM)
    smem = pl.BlockSpec(memory_space=pltpu.SMEM)
    i32 = jnp.int32
    dma = pltpu.SemaphoreType.DMA

    def vmem(shape, kind=f32):
        return pltpu.VMEM(shape, kind)

    loaded = (
        positions, velocities, charges, inverse_mass, export_rows, partners, bond_partners, bond_rest, block_offsets,
    )
    constants = (halves(dealt), halves(cas), halves(wide), halves(wide.T), jnp.asarray(along), jnp.asarray(across))
    tile = (8, LANES)
    kernel = functools.partial(
        program_kernel, tiles=tiles, pens=pens, subs=subs, planes=planes, deep=deep, share=share, lows=lows,
        chunk=chunk, keep=keep,
    )
    return pl.pallas_call(
        kernel,
        out_shape=(
            jax.ShapeDtypeStruct(positions.shape, f32),
            jax.ShapeDtypeStruct(velocities.shape, f32),
            jax.ShapeDtypeStruct((1, 1, width), f32),
        ),
        in_specs=[smem] * 2 + [hbm] * (len(loaded) + len(constants)),
        out_specs=(hbm, hbm, hbm),
        scratch_shapes=[vmem(x.shape, x.dtype) for x in loaded]
        + [vmem((2, share, GRID), bf16)]
        + [vmem(x.shape, x.dtype) for x in constants[1:]]
        + [
            vmem((subs, slots, width), i32), vmem((subs, bond_rows, width), i32), vmem((subs, bond_rows, width)),
            vmem((chunks,) + tile), vmem((INNER, 4, LANES)), vmem((INNER, near, subs, 4, LANES)),
            vmem((INNER, chunks, 4, LANES)), vmem((INNER, subs, chunks, 4, LANES)),
            vmem((group, 4, width)), vmem((group, 4, width)), vmem((4, width)), vmem((subs, 4, width)),
            vmem((chunks, groups) + tile, i32), vmem((chunks, groups) + tile, i32),
            vmem((chunks, groups) + tile), vmem((chunks, groups) + tile), vmem((chunks, groups) + tile),
            vmem((chunks, groups, 3) + tile), vmem((chunks, 3) + tile),
            vmem((chunks, bond_tiles) + tile, i32), vmem((chunks, bond_tiles) + tile),
            vmem((share, GRID + 8, GRID)), vmem((tiles, deep, wide_atoms)), vmem((tiles, share, wide_atoms)),
            vmem((share, wide_atoms)), vmem((tiles if keep else 1, 2, GRID, wide_atoms), bf16),
            vmem((group, 1, width)), vmem((group, 1, width)),
            vmem(positions.shape), vmem(velocities.shape), vmem((1, 1, width)),
            dma((18,)), dma((3,)), dma((INNER, near, subs)), dma((INNER, near, subs)),
            dma((INNER, subs)), dma((INNER, subs)), dma((4, subs)), dma((4, subs)),
            dma((group,)), dma((group,)), dma((group,)), dma((group,)), dma((group,)), dma((group,)),
        ],
        compiler_params=pltpu.CompilerParams(
            collective_id=0, has_side_effects=True, vmem_limit_bytes=60 * 1024 * 1024
        ),
    )(jnp.asarray(line), jnp.asarray(square), *loaded, *constants)


def solution(mesh):
    placed = (
        P("rep", "tile", "pen", None),
        P("rep", "tile", "pen", None),
        P(("rep", "tile"), "pen", None),
        P(("rep", "tile"), "pen", None),
        P(("rep", "tile"), "pen", None),
        P(("rep", "tile"), "pen", "sub", None),
        P(("rep", "tile"), "pen", "sub", None),
        P(("rep", "tile"), "pen", "sub", None),
        P("rep", "tile", "pen", None),
    )
    return jax.shard_map(
        on_device,
        mesh=mesh,
        in_specs=placed,
        out_specs=(
            P("rep", "tile", "pen", None),
            P("rep", "tile", "pen", None),
            P(("rep", "tile"), "pen", "sub"),
        ),
        check_vma=False,
    )
```

```python
import functools
import math

import jax
import jax.numpy as jnp
import numpy as np
from jax import lax
from jax.experimental import pallas as pl
from jax.experimental.pallas import tpu as pltpu
from jax.sharding import PartitionSpec as P

GRID = 256
INNER = 4
LANES = 128
LOW = 128
BATCH = 4

time_step = 0.1
coulomb = 30.0
bond_stiffness = 0.2
soften = 1.0
cutoff_sq = 144.0
ewald_beta = 0.32

f32 = jnp.float32
bf16 = jnp.bfloat16


def lane_gather(rows, low):
    return jnp.take_along_axis(rows, low, axis=1, mode="promise_in_bounds")


def split(value):
    high = value.astype(bf16)
    return high, (value - high.astype(f32)).astype(bf16)


def single(left, right, turned=False):
    dims = (((1,), (1 if turned else 0,)), ((), ()))
    return lax.dot_general(left, right, dims, preferred_element_type=f32)


def product(left, right, turned=False):
    return single(left[0], right[0], turned) + (
        single(left[0], right[1], turned) + single(left[1], right[0], turned)
    )


def half_product(left, right, turned=False):
    return single(left[0], right, turned) + single(left[1], right, turned)


def spline(place, frac):
    rest = 1.0 - frac
    square = frac * frac
    cube = square * frac
    pieces = (
        rest * rest * rest / 6.0,
        (3.0 * cube - 6.0 * square + 4.0) / 6.0,
        (-3.0 * cube + 3.0 * square + 3.0 * frac + 1.0) / 6.0,
        cube / 6.0,
    )
    total = jnp.zeros(place.shape, f32)
    for order in range(4):
        total = jnp.where(place == order, pieces[order], total)
    return total


def wide_row(row):
    return jnp.broadcast_to(row, (8, LANES))


def stacked(rows):
    place = lax.broadcasted_iota(jnp.int32, (8, LANES), 0)
    total = jnp.zeros((8, LANES), rows[0].dtype)
    for r, row in enumerate(rows):
        total = jnp.where(place == r, wide_row(row), total)
    return total


def program_kernel(
    lines_ref, squares_ref,
    pos_hbm, vel_hbm, chg_hbm, imass_hbm, shown_hbm, parts_hbm, bonds_hbm, rest_hbm, offs_hbm,
    mine_hbm, cas_hbm, wide_hbm, tall_hbm, along_hbm, across_hbm,
    out_hbm,
    pos_in, vel_in, chg_in, imass_in, shown_in, parts_in, bonds_in, rest_in, offs_in,
    mine_ref, cas_ref, wide_ref, tall_ref, along_ref, across_ref,
    parts_all, bonds_all, rest_all,
    mine, sent, beside, half_sent, half_recv, static_all, pos_all, vel_sent, vel_far,
    low_ref, blk_ref, shx_ref, shy_ref, qq_ref, near_ref, bforce, bidx_ref, brest_ref,
    grid, wx, wy, wyq, wz, part_sent, part_recv, out_fin,
    load_sem, out_sem, step_send, step_recv, half_send_sem, half_recv_sem,
    pair_send, pair_recv, static_send, static_recv, place_send, place_recv, part_send_sem, part_recv_sem,
    *, tiles, pens, subs, planes, deep, share, lows, chunk, keep,
):
    ti, pi, si = lax.axis_index("tile"), lax.axis_index("pen"), lax.axis_index("sub")
    local = pens * subs
    group = tiles * local
    me = (ti * pens + pi) * subs + si
    atoms = pos_in.shape[3]
    width = atoms // subs
    chunks = width // LANES
    own_blocks = atoms // LANES
    slots = parts_all.shape[1]
    groups = subs * slots // 8
    bond_rows = bonds_all.shape[1]

    offsets = []
    for i in range(3):
        for j in range(3):
            step = ((i - 1) % tiles, (j - 1) % pens)
            if step != (0, 0) and step not in offsets:
                offsets.append(step)

    def remote(src, dst, send, recv, device):
        return pltpu.make_async_remote_copy(
            src_ref=src, dst_ref=dst, send_sem=send, recv_sem=recv,
            device_id=device, device_id_type=pl.DeviceIdType.MESH,
        )

    def tile_at(s):
        if tiles & (tiles - 1):
            return lax.rem(ti + s, tiles)
        total, bit = 0, 1
        while bit < tiles:
            total = total + lax.rem(lax.rem(lax.div(ti, bit), 2) + lax.rem(lax.div(s, bit), 2), 2) * bit
            bit *= 2
        return total

    def peer(d):
        s, rest = lax.div(d, local), lax.rem(d, local)
        t = tile_at(s)
        p = lax.rem(pi + lax.div(rest, subs), pens)
        q = lax.rem(si + lax.rem(rest, subs), subs)
        return {"tile": t, "pen": p, "sub": q}, (t * pens + p) * subs + q

    def each_peer(body):
        def step(d, carry):
            body(d, *peer(d))
            return carry

        lax.fori_loop(1, group, step, 0)

    half_lanes = pl.ds(pl.multiple_of(si * width, LANES), width)
    first_loads = [
        (parts_hbm.at[0, 0, :, half_lanes], parts_all.at[si]),
        (bonds_hbm.at[0, 0, :, half_lanes], bonds_all.at[si]),
        (rest_hbm.at[0, 0, :, half_lanes], rest_all.at[si]),
        (parts_hbm, parts_in), (bonds_hbm, bonds_in), (rest_hbm, rest_in),
        (pos_hbm, pos_in), (vel_hbm, vel_in), (chg_hbm, chg_in), (imass_hbm, imass_in),
        (shown_hbm, shown_in), (offs_hbm, offs_in),
    ]
    later_loads = [
        (mine_hbm.at[:, me], mine_ref), (cas_hbm, cas_ref), (wide_hbm, wide_ref), (tall_hbm, tall_ref),
        (along_hbm, along_ref), (across_hbm, across_ref),
    ]
    loads = [
        pltpu.make_async_copy(src, dst, load_sem.at[k]) for k, (src, dst) in enumerate(first_loads + later_loads)
    ]
    for copy in loads:
        copy.start()

    barrier = pltpu.get_barrier_semaphore()

    def greet(d, device, g):
        pl.semaphore_signal(barrier, inc=1, device_id=device, device_id_type=pl.DeviceIdType.MESH)

    each_peer(greet)
    for copy in loads[: len(first_loads)]:
        copy.wait()

    for c in range(chunks):
        lanes = pl.ds(pl.multiple_of(si * width + c * LANES, LANES), LANES)
        rows = [pos_in[r, 0, :, lanes] for r in range(3)] + [chg_in[0, :, lanes]]
        rows += [vel_in[r, 0, :, lanes] for r in range(3)] + [imass_in[0, :, lanes]]
        mine[c] = stacked(rows)
        offset = stacked([offs_in[r, 0, :, lanes].astype(f32) for r in range(3)])
        static_all[me, :, c * LANES : (c + 1) * LANES] = offset[:4]
    for step in range(1, subs):
        other = lax.rem(si + step, subs)
        for c in range(chunks):
            lanes = pl.ds(pl.multiple_of(other * width + c * LANES, LANES), LANES)
            half_recv[0, other, c] = stacked([pos_in[r, 0, :, lanes] for r in range(3)] + [chg_in[0, :, lanes]])[:4]

    shown = jnp.broadcast_to(shown_in[0], (8, LANES))
    shown_low, shown_high = shown & (LANES - 1), shown >> 7

    def step_copy(n, slot, q):
        dt, dp = offsets[slot]
        back = offsets.index(((-dt) % tiles, (-dp) % pens))
        device = {"tile": lax.rem(ti + dt, tiles), "pen": lax.rem(pi + dp, pens), "sub": q}
        return remote(sent.at[n], beside.at[n, back, si], step_send.at[n, slot, q], step_recv.at[n, back, si], device)

    def half_copy(n, step):
        other = lax.rem(si + step, subs)
        return remote(
            half_sent.at[n], half_recv.at[n, si], half_send_sem.at[n, step], half_recv_sem.at[n, si], {"sub": other}
        )

    def show(n):
        total = jnp.zeros((8, LANES), f32)
        for c in range(chunks):
            total = jnp.where(shown_high == si * chunks + c, lane_gather(mine[c], shown_low), total)
        sent[n] = total[:4]

    def send_shown(n):
        for slot in reversed(range(len(offsets))):
            for q in range(subs):
                step_copy(n, slot, q).start()

    def wait_shown(n):
        for slot in range(len(offsets)):
            for q in range(subs):
                remote(
                    sent.at[n], beside.at[n, slot, q], step_send.at[n, slot, q], step_recv.at[n, slot, q], {"sub": si}
                ).wait_recv()
                step_copy(n, slot, q).wait_send()

    show(0)
    pl.semaphore_wait(barrier, group - 1)
    send_shown(0)
    pairs = []
    for step in range(1, subs):
        other = lax.rem(si + step, subs)
        lanes = pl.ds(pl.multiple_of(other * width, LANES), width)
        for k, (source, target) in enumerate(
            ((parts_in, parts_all), (bonds_in, bonds_all), (rest_in, rest_all))
        ):
            pairs.append((k, step, source.at[0, 0, :, lanes], target, other))
    for k, step, source, target, other in pairs:
        remote(source, target.at[si], pair_send.at[k, step], pair_recv.at[k, si], {"sub": other}).start()

    def static_copy(d, device):
        return remote(static_all.at[me], static_all.at[me], static_send.at[d], static_recv.at[me], device)

    each_peer(lambda d, device, g: static_copy(d, device).start())
    for k, step, source, target, other in pairs:
        remote(source, target.at[other], pair_send.at[k, step], pair_recv.at[k, other], {"sub": other}).wait_recv()
        remote(source, target.at[si], pair_send.at[k, step], pair_recv.at[k, si], {"sub": other}).wait_send()

    moves_x, moves_y = [], []
    for i in range(3):
        near = ti + (i - 1)
        moves_x.append(jnp.where(near < 0, -float(GRID), jnp.where(near >= tiles, float(GRID), 0.0)))
        near = pi + (i - 1)
        moves_y.append(jnp.where(near < 0, -float(GRID), jnp.where(near >= pens, float(GRID), 0.0)))
    for c in range(chunks):
        for g in range(groups):
            q, row = divmod(g * 8, slots)
            index = parts_all[q, row : row + 8, c * LANES : (c + 1) * LANES]
            high = index >> 7
            block = high
            shx = jnp.zeros((8, LANES), f32)
            shy = jnp.zeros((8, LANES), f32)
            for i in range(3):
                for j in range(3):
                    if (i, j) == (1, 1):
                        continue
                    hit = high == own_blocks + i * 3 + j
                    step = ((i - 1) % tiles, (j - 1) % pens)
                    block = jnp.where(hit, own_blocks + offsets.index(step), block)
                    if i != 1:
                        shx = jnp.where(hit, moves_x[i], shx)
                    if j != 1:
                        shy = jnp.where(hit, moves_y[j], shy)
            low_ref[c, g] = index & (LANES - 1)
            blk_ref[c, g] = block
            shx_ref[c, g] = shx
            shy_ref[c, g] = shy
        atom = lax.broadcasted_iota(jnp.int32, (1, LANES), 1) + (si * width + c * LANES)
        every = [(q, b) for q in range(subs) for b in range(bond_rows)]
        for v in range(bidx_ref.shape[1]):
            part = every[v * 8 : v * 8 + 8]
            lanes = slice(c * LANES, (c + 1) * LANES)
            rows = [bonds_all[q, b : b + 1, lanes] for q, b in part]
            rows += [atom] * (8 - len(part))
            bidx_ref[c, v] = stacked(rows)
            brest_ref[c, v] = stacked([rest_all[q, b : b + 1, lanes] for q, b in part])

    def own_tables(rows):
        out = []
        for c in range(chunks):
            out.append((si * chunks + c, [wide_row(mine[c, r : r + 1, :]) for r in rows]))
        return out

    def far_tables(n, rows):
        out = []
        for step in range(1, subs):
            other = lax.rem(si + step, subs)
            for c in range(chunks):
                out.append((other * chunks + c, [wide_row(half_recv[n, other, c, r : r + 1, :]) for r in rows]))
        return out

    def around_tables(n, rows):
        out = []
        for slot in range(len(offsets)):
            patch = beside[n, slot, 0]
            for q in range(1, subs):
                patch = patch + beside[n, slot, q]
            out.append((own_blocks + slot, [wide_row(patch[r : r + 1, :]) for r in rows]))
        return out

    def pick(found, low, block, table):
        for number, sources in table:
            hit = block == number
            found = [jnp.where(hit, lane_gather(source, low), f) for source, f in zip(sources, found)]
        return found

    xyz = (0, 1, 2)

    def near_part(n, wait):
        table = own_tables(xyz)
        for c in range(chunks):
            for g in range(groups):
                found = pick([jnp.zeros((8, LANES), f32)] * 3, low_ref[c, g], blk_ref[c, g], table)
                for r in xyz:
                    near_ref[c, g, r] = found[r]
        if wait:
            for step in range(1, subs):
                other = lax.rem(si + step, subs)
                remote(
                    half_sent.at[n], half_recv.at[n, other], half_send_sem.at[n, step], half_recv_sem.at[n, other],
                    {"sub": other},
                ).wait_recv()
                half_copy(n, step).wait_send()
        more = far_tables(n, xyz)
        for c in range(chunks):
            for g in range(groups):
                found = [near_ref[c, g, r] for r in xyz]
                found = pick(found, low_ref[c, g], blk_ref[c, g], more)
                for r in xyz:
                    near_ref[c, g, r] = found[r]
            own = [wide_row(mine[c, r : r + 1, :]) for r in xyz]
            force = [jnp.zeros((8, LANES), f32)] * 3
            for v in range(bidx_ref.shape[1]):
                index = bidx_ref[c, v]
                near = pick([jnp.zeros((8, LANES), f32)] * 3, index & (LANES - 1), index >> 7, table + more)
                delta = [own[r] - near[r] for r in xyz]
                root = lax.rsqrt(delta[0] * delta[0] + delta[1] * delta[1] + delta[2] * delta[2] + soften)
                pull = -bond_stiffness * (1.0 - brest_ref[c, v] * root)
                force = [force[r] + pull * delta[r] for r in xyz]
            for r in xyz:
                bforce[c, r] = force[r]

    def far_part(n):
        table = around_tables(n, xyz)
        for c in range(chunks):
            own = [wide_row(mine[c, r : r + 1, :]) for r in xyz]
            force = [bforce[c, r] for r in xyz]
            for g in range(groups):
                near = pick([near_ref[c, g, r] for r in xyz], low_ref[c, g], blk_ref[c, g], table)
                delta = [own[0] - (near[0] + shx_ref[c, g]), own[1] - (near[1] + shy_ref[c, g]), own[2] - near[2]]
                dist_sq = delta[0] * delta[0] + delta[1] * delta[1] + delta[2] * delta[2]
                taper = 1.0 - dist_sq * (1.0 / cutoff_sq)
                taper = jnp.where(dist_sq < cutoff_sq, taper * taper, 0.0)
                root = lax.rsqrt(dist_sq + soften)
                strength = qq_ref[c, g] * taper * (root * root * root)
                force = [force[r] + strength * delta[r] for r in xyz]
            scale = mine[c, 7:8, :]
            for r in xyz:
                total = jnp.sum(force[r], axis=0, keepdims=True)
                speed = mine[c, 4 + r : 5 + r, :] + time_step * scale * total
                mine[c, 4 + r : 5 + r, :] = speed
                mine[c, r : r + 1, :] = mine[c, r : r + 1, :] + time_step * speed

    near_part(0, False)
    wait_shown(0)
    table = own_tables((3,)) + far_tables(0, (3,)) + around_tables(0, (3,))
    for c in range(chunks):
        own = wide_row(mine[c, 3:4, :])
        for g in range(groups):
            (near,) = pick([jnp.zeros((8, LANES), f32)], low_ref[c, g], blk_ref[c, g], table)
            qq_ref[c, g] = coulomb * own * near

    def inner(n, carry):
        far_part(n)
        for c in range(chunks):
            half_sent[n + 1, c] = mine[c][:4]
        show(n + 1)
        for step in range(1, subs):
            half_copy(n + 1, step).start()
        send_shown(n + 1)
        near_part(n + 1, True)
        wait_shown(n + 1)
        return carry

    lax.fori_loop(0, INNER - 1, inner, 0)
    far_part(INNER - 1)

    for c in range(chunks):
        lanes = slice(c * LANES, (c + 1) * LANES)
        pos_all[me, :, lanes] = mine[c][:4]
        vel_sent[:, lanes] = mine[c][4:]

    def place_copy(d, device):
        return remote(pos_all.at[me], pos_all.at[me], place_send.at[d], place_recv.at[me], device)

    def place_wait(g):
        remote(pos_all.at[me], pos_all.at[g], place_send.at[0], place_recv.at[g], {"sub": si}).wait_recv()

    def speed_copy(step):
        other = lax.rem(si + step, subs)
        return remote(vel_sent, vel_far.at[si], pair_send.at[3, step], pair_recv.at[3, si], {"sub": other})

    each_peer(lambda d, device, g: place_copy(d, device).start())
    for step in range(1, subs):
        speed_copy(step).start()

    for copy in loads[len(first_loads) :]:
        copy.wait()
    each_peer(
        lambda d, device, g: remote(
            static_all.at[me], static_all.at[g], static_send.at[d], static_recv.at[g], {"sub": si}
        ).wait_recv()
    )
    each_peer(lambda d, device, g: static_copy(d, device).wait_send())
    wide_atoms = local * width
    top = tiles * planes

    def cells(offset, count):
        return lax.broadcasted_iota(jnp.int32, (count, wide_atoms), 0) - offset

    def row_of(ref, t, r):
        return jnp.concatenate([ref[t * local + q, r : r + 1, :] for q in range(local)], axis=1)

    def prepare(t, r):
        offset = row_of(static_all, t, r)
        return offset.astype(jnp.int32), row_of(pos_all, t, r) - (offset + 1.0)

    def depth_of(t):
        offset, frac = prepare(t, 2)
        depth = spline(cells(offset, GRID) & (GRID - 1), frac)
        return split(product((cas_ref[0], cas_ref[1]), split(depth)))

    def clear(j, carry):
        for edge in range(tiles + 1):
            grid[j, edge * planes : edge * planes + 8] = jnp.zeros((8, GRID), f32)
        return carry

    lax.fori_loop(0, share, clear, 0)
    parts = [(c, min(c + chunk, lows), True) for c in range(0, lows, chunk)]
    parts += [(c, min(c + chunk, share), False) for c in range(lows, share, chunk)]

    def spread(s, carry):
        t = tile_at(s)

        def arrived(q, inner_carry):
            place_wait(t * local + lax.rem(pi * subs + si + q, local))
            return inner_carry

        @pl.when(s > 0)
        def _():
            place_wait(t * local + pi * subs + si)

        lax.fori_loop(1, local, arrived, 0)
        offset, frac = prepare(t, 0)
        wx[t] = spline(cells(offset - (t * planes - 1), deep), frac)
        offset, frac = prepare(t, 1)
        rows = spline(cells(offset, GRID) & (GRID - 1), frac)
        wy[t] = product((mine_ref[0], mine_ref[1]), split(rows))
        wyq[...] = wy[t] * row_of(pos_all, t, 3)
        depth = depth_of(t)
        if keep:
            wz[t, 0] = depth[0]
            wz[t, 1] = depth[1]
        base = pl.multiple_of(t * planes, 8)
        for start, stop, exact in parts:
            plane = jnp.concatenate([wx[t] * wyq[k : k + 1, :] for k in range(start, stop)], axis=0)
            if exact:
                values = product(split(plane), depth, True)
            else:
                values = single(plane.astype(bf16), depth[0], True)
            values = values.reshape(stop - start, deep, GRID)
            for k in range(start, stop):
                value = values[k - start]
                grid[k, pl.ds(base, 8)] += value[:8]
                if planes > 8:
                    grid[k, pl.ds(pl.multiple_of(base + 8, 8), planes - 8)] = value[8:planes]
                grid[k, pl.ds(pl.multiple_of(base + planes, 8), 8)] += value[planes : planes + 8]
        return carry


    lax.fori_loop(0, tiles, spread, 0)
    for r in range(3):
        for q in range(subs):
            lanes = slice(q * width, (q + 1) * width)
            out_fin[r, :, lanes] = pos_all[(ti * pens + pi) * subs + q, r : r + 1, :]
    for step in range(1, subs):
        other = lax.rem(si + step, subs)
        remote(
            vel_sent, vel_far.at[other], pair_send.at[3, step], pair_recv.at[3, other], {"sub": other}
        ).wait_recv()
        speed_copy(step).wait_send()
        lanes = pl.ds(pl.multiple_of(other * width, LANES), width)
        for r in range(3):
            out_fin[3 + r, :, lanes] = vel_far[other, r : r + 1, :]
    for r in range(3):
        out_fin[3 + r, :, half_lanes] = vel_sent[r : r + 1, :]

    def transform(start, stop, exact):
        batch = math.gcd(math.gcd(start, stop), BATCH)

        def step(n, carry):
            first = start + n * batch
            lines = []
            for i in range(batch):
                line = grid[first + i, 0:top]
                edge = line[:8] + grid[first + i, top : top + 8]
                lines.append(jnp.concatenate([edge, line[8:]], axis=0))
            line = split(jnp.concatenate(lines, axis=1))
            spectrum = product((wide_ref[0], wide_ref[1]), line)
            weighted = []
            for i in range(batch):
                m_sq = along_ref[...] + squares_ref[me * share + first + i]
                anchor = m_sq == 0.0
                value = across_ref[...] * lines_ref[me * share + first + i] / jnp.where(anchor, 1.0, m_sq)
                weighted.append(spectrum[:, i * GRID : (i + 1) * GRID] * jnp.where(anchor, 0.0, value))
            weighted = jnp.concatenate(weighted, axis=1)
            if exact:
                back = product((tall_ref[0], tall_ref[1]), split(weighted))
            else:
                back = half_product((tall_ref[0], tall_ref[1]), weighted.astype(bf16))
            for i in range(batch):
                grid[first + i, 0:top] = back[:, i * GRID : (i + 1) * GRID]
                grid[first + i, top : top + 8] = back[0:8, i * GRID : (i + 1) * GRID]
            return carry

        if stop > start:
            lax.fori_loop(0, (stop - start) // batch, step, 0)

    transform(0, lows, True)
    transform(lows, share, False)

    def part_copy(g, device):
        return remote(part_sent.at[g], part_recv.at[me], part_send_sem.at[g], part_recv_sem.at[me], device)

    def device_of(g):
        return {"tile": lax.div(g, local), "pen": lax.rem(lax.div(g, subs), pens), "sub": lax.rem(g, subs)}

    def read(n, carry):
        s = tiles - 1 - n
        t = tile_at(s)
        if keep:
            depth = (wz[t, 0], wz[t, 1])
        else:
            depth = depth_of(t)
        base = pl.multiple_of(t * planes, 8)
        total = jnp.zeros((planes + 8, wide_atoms), f32)
        for start, stop, exact in parts:
            rows = [grid[k, pl.ds(base, planes + 8)] for k in range(start, stop)]
            line = jnp.concatenate(rows, axis=0)
            if exact:
                values = product(split(line), depth)
            else:
                values = single(line.astype(bf16), depth[0])
            for k in range(start, stop):
                part = values[(k - start) * (planes + 8) : (k - start + 1) * (planes + 8)]
                total = total + part * wy[t, k : k + 1, :]
        result = jnp.sum(total * wx[t, : planes + 8], axis=0, keepdims=True)
        for q in range(local):
            part_sent[t * local + q] = result[:, q * width : (q + 1) * width]

        @pl.when(s > 0)
        def _():
            g = t * local + pi * subs + si
            part_copy(g, device_of(g)).start()

        def give(q, inner_carry):
            g = t * local + lax.rem(pi * subs + si + q, local)
            part_copy(g, device_of(g)).start()
            return inner_carry

        lax.fori_loop(1, local, give, 0)
        return carry

    lax.fori_loop(0, tiles, read, 0)
    part_recv[me] = part_sent[me]
    each_peer(lambda d, device, g: place_copy(d, device).wait_send())
    each_peer(lambda d, device, g: part_copy(g, device).wait_send())
    each_peer(
        lambda d, device, g: remote(
            part_sent.at[me], part_recv.at[g], part_send_sem.at[g], part_recv_sem.at[g], {"sub": si}
        ).wait_recv()
    )
    out_fin[6, :, 0:width] = jnp.sum(part_recv[...], axis=0)
    out_fin[6, :, width:] = jnp.zeros((1, atoms - width), f32)
    last = pltpu.make_async_copy(out_fin, out_hbm, out_sem.at[0])
    last.start()
    last.wait()


def halves(table):
    table = jnp.asarray(table.astype(np.float32))
    return jnp.stack(split(table))


def tables(group):
    share = GRID // group
    index = np.arange(GRID)
    angle = 2.0 * math.pi / GRID * np.mod(index[:, None] * index[None, :], GRID)
    cas = np.cos(angle) + np.sin(angle)
    wide = cas[:, np.mod(index - 1, GRID)]
    order = np.array([(r + 1) // 2 if r % 2 else (GRID - r // 2) % GRID for r in range(GRID)])
    dealt = order.reshape(share, group).T
    signed = np.where(index > GRID // 2, index - GRID, index).astype(np.float64)
    turn = 2.0 * math.pi / GRID * index
    real = (1.0 + 4.0 * np.cos(turn) + np.cos(2.0 * turn)) / 6.0
    imag = (4.0 * np.sin(turn) + np.sin(2.0 * turn)) / 6.0
    square = signed**2 / float(GRID * GRID)
    line = np.exp(-((math.pi / ewald_beta) ** 2) * square) / (real * real + imag * imag)
    along = square[:, None] + square[None, :]
    across = line[:, None] * line[None, :] / (math.pi * float(GRID) ** 3)
    flat = dealt.reshape(-1)
    return (
        cas, wide, cas[dealt], line[flat].astype(np.float32), square[flat].astype(np.float32),
        along.astype(np.float32), across.astype(np.float32),
    )


def on_device(
    positions, velocities, charges, inverse_mass, export_rows, partners, bond_partners, bond_rest, block_offsets,
):
    tiles, pens, subs = lax.axis_size("tile"), lax.axis_size("pen"), lax.axis_size("sub")
    local = pens * subs
    group = tiles * local
    atoms, exported = positions.shape[3], export_rows.shape[2]
    slots, bond_rows = partners.shape[2], bond_partners.shape[2]
    width = atoms // subs
    chunks = width // LANES
    groups = subs * slots // 8
    planes = GRID // tiles
    share = GRID // group
    lows = min(share, max(1, -(-LOW // group)))
    chunk = math.gcd(share, 4)
    unit = 8 if chunk % 2 == 0 else 16
    deep = -(-(planes + 8) // unit) * unit
    wide_atoms = local * width
    keep = group * width * GRID * 4 <= 16 * 1024 * 1024
    cas, wide, dealt, line, square, along, across = tables(group)
    around = {((i - 1) % tiles, (j - 1) % pens) for i in range(3) for j in range(3)} - {(0, 0)}
    near = len(around)
    bond_tiles = -(-subs * bond_rows // 8)
    assert exported == LANES and slots % 8 == 0 and planes % 8 == 0
    hbm = pl.BlockSpec(memory_space=pltpu.HBM)
    smem = pl.BlockSpec(memory_space=pltpu.SMEM)
    i32 = jnp.int32
    dma = pltpu.SemaphoreType.DMA

    def vmem(shape, kind=f32):
        return pltpu.VMEM(shape, kind)

    loaded = (
        positions, velocities, charges, inverse_mass, export_rows, partners, bond_partners, bond_rest, block_offsets,
    )
    constants = (halves(dealt), halves(cas), halves(wide), halves(wide.T), jnp.asarray(along), jnp.asarray(across))
    tile = (8, LANES)
    kernel = functools.partial(
        program_kernel, tiles=tiles, pens=pens, subs=subs, planes=planes, deep=deep, share=share, lows=lows,
        chunk=chunk, keep=keep,
    )
    out = pl.pallas_call(
        kernel,
        out_shape=jax.ShapeDtypeStruct((7, 1, atoms), f32),
        in_specs=[smem] * 2 + [hbm] * (len(loaded) + len(constants)),
        out_specs=hbm,
        scratch_shapes=[vmem(x.shape, x.dtype) for x in loaded]
        + [vmem((2, share, GRID), bf16)]
        + [vmem(x.shape, x.dtype) for x in constants[1:]]
        + [
            vmem((subs, slots, width), i32), vmem((subs, bond_rows, width), i32), vmem((subs, bond_rows, width)),
            vmem((chunks,) + tile), vmem((INNER, 4, LANES)), vmem((INNER, near, subs, 4, LANES)),
            vmem((INNER, chunks, 4, LANES)), vmem((INNER, subs, chunks, 4, LANES)),
            vmem((group, 4, width)), vmem((group, 4, width)), vmem((4, width)), vmem((subs, 4, width)),
            vmem((chunks, groups) + tile, i32), vmem((chunks, groups) + tile, i32),
            vmem((chunks, groups) + tile), vmem((chunks, groups) + tile), vmem((chunks, groups) + tile),
            vmem((chunks, groups, 3) + tile), vmem((chunks, 3) + tile),
            vmem((chunks, bond_tiles) + tile, i32), vmem((chunks, bond_tiles) + tile),
            vmem((share, GRID + 8, GRID)), vmem((tiles, deep, wide_atoms)), vmem((tiles, share, wide_atoms)),
            vmem((share, wide_atoms)), vmem((tiles if keep else 1, 2, GRID, wide_atoms), bf16),
            vmem((group, 1, width)), vmem((group, 1, width)),
            vmem((7, 1, atoms)),
            dma((18,)), dma((3,)), dma((INNER, near, subs)), dma((INNER, near, subs)),
            dma((INNER, subs)), dma((INNER, subs)), dma((4, subs)), dma((4, subs)),
            dma((group,)), dma((group,)), dma((group,)), dma((group,)), dma((group,)), dma((group,)),
        ],
        compiler_params=pltpu.CompilerParams(
            collective_id=0, has_side_effects=True, vmem_limit_bytes=60 * 1024 * 1024
        ),
    )(jnp.asarray(line), jnp.asarray(square), *loaded, *constants)
    return out[0:3].reshape(positions.shape), out[3:6].reshape(velocities.shape), out[6:7, :, :width]


def solution(mesh):
    placed = (
        P("rep", "tile", "pen", None),
        P("rep", "tile", "pen", None),
        P(("rep", "tile"), "pen", None),
        P(("rep", "tile"), "pen", None),
        P(("rep", "tile"), "pen", None),
        P(("rep", "tile"), "pen", "sub", None),
        P(("rep", "tile"), "pen", "sub", None),
        P(("rep", "tile"), "pen", "sub", None),
        P("rep", "tile", "pen", None),
    )
    return jax.shard_map(
        on_device,
        mesh=mesh,
        in_specs=placed,
        out_specs=(
            P("rep", "tile", "pen", None),
            P("rep", "tile", "pen", None),
            P(("rep", "tile"), "pen", "sub"),
        ),
        check_vma=False,
    )
```

```python
import functools
import math

import jax
import jax.numpy as jnp
import numpy as np
from jax import lax
from jax.experimental import pallas as pl
from jax.experimental.pallas import tpu as pltpu
from jax.sharding import PartitionSpec as P

GRID = 256
INNER = 4
LANES = 128
LOW = 128
BATCH = 8
VMEM_LIMIT = 60 * 1024 * 1024

time_step = 0.1
coulomb = 30.0
bond_stiffness = 0.2
soften = 1.0
cutoff_sq = 144.0
ewald_beta = 0.32

f32 = jnp.float32
bf16 = jnp.bfloat16


def lane_gather(rows, low):
    return jnp.take_along_axis(rows, low, axis=1, mode="promise_in_bounds")


def split(value):
    high = value.astype(bf16)
    return high, (value - high.astype(f32)).astype(bf16)


def single(left, right, turned=False):
    dims = (((1,), (1 if turned else 0,)), ((), ()))
    return lax.dot_general(left, right, dims, preferred_element_type=f32)


def product(left, right, turned=False):
    return single(left[0], right[0], turned) + (
        single(left[0], right[1], turned) + single(left[1], right[0], turned)
    )


def half_product(left, right, turned=False):
    return single(left[0], right, turned) + single(left[1], right, turned)


def spline_pieces(frac):
    rest = 1.0 - frac
    square = frac * frac
    cube = square * frac
    sixth = 1.0 / 6.0
    return (
        rest * rest * rest * sixth,
        (3.0 * cube - 6.0 * square + 4.0) * sixth,
        (-3.0 * cube + 3.0 * square + 3.0 * frac + 1.0) * sixth,
        cube * sixth,
    )


def spline(place, frac):
    pieces = spline_pieces(frac)
    total = jnp.zeros(place.shape, f32)
    for order in range(4):
        total = jnp.where(place == order, pieces[order], total)
    return total


def wide_row(row):
    return jnp.broadcast_to(row, (8, LANES))


def stacked(rows):
    place = lax.broadcasted_iota(jnp.int32, (8, LANES), 0)
    total = jnp.zeros((8, LANES), rows[0].dtype)
    for r, row in enumerate(rows):
        total = jnp.where(place == r, wide_row(row), total)
    return total


def program_kernel(
    pos_hbm, vel_hbm, chg_hbm, imass_hbm, shown_hbm, parts_hbm, bonds_hbm, rest_hbm, offs_hbm,
    mine_hbm, cas_hbm, tall_hbm, along_hbm, across_hbm, freq_hbm,
    out_ref,
    pos_in, vel_in, chg_in, imass_in, shown_in, parts_all, bonds_all, rest_all, offs_in,
    mine_ref, cas_ref, tall_ref, along_ref, across_ref, freq_ref,
    mine, sent, beside, static_all, pos_all, speeds,
    low_ref, blk_ref, shx_ref, shy_ref, qq_ref, near_ref, bforce, bidx_ref, brest_ref,
    grid, wx, wy, wyq, wz, gz, gy, part_sent, part_recv,
    load_sem, step_send, step_recv, pair_send, pair_recv,
    static_send, static_recv, place_send, place_recv, part_send_sem, part_recv_sem,
    *, tiles, pens, subs, planes, deep, share, lows, chunk, keep,
):
    ti, pi, si = lax.axis_index("tile"), lax.axis_index("pen"), lax.axis_index("sub")
    lead = subs - 1
    leads = si == lead
    local = pens * subs
    group = tiles * local
    patch = ti * pens + pi
    me = patch * subs + si
    atoms = pos_in.shape[3]
    width = atoms // subs
    chunks = atoms // LANES
    shown_chunk = chunks
    slots = parts_all.shape[1]
    groups = subs * slots // 8
    bond_rows = bonds_all.shape[1]
    everyone = range(chunks + 1)

    offsets = []
    for i in range(3):
        for j in range(3):
            step = ((i - 1) % tiles, (j - 1) % pens)
            if step != (0, 0) and step not in offsets:
                offsets.append(step)

    def remote(src, dst, send, recv, device):
        return pltpu.make_async_remote_copy(
            src_ref=src, dst_ref=dst, send_sem=send, recv_sem=recv,
            device_id=device, device_id_type=pl.DeviceIdType.MESH,
        )

    def shifted(index, step, count):
        if isinstance(step, int):
            moved = index + step % count
            return moved if step % count == 0 else jnp.where(moved >= count, moved - count, moved)
        return lax.rem(index + step, count)

    bits = []
    if tiles & (tiles - 1) == 0:
        bits = [lax.rem(lax.div(ti, 1 << b), 2) for b in range(tiles.bit_length() - 1)]

    def tile_at(s):
        if tiles & (tiles - 1):
            return shifted(ti, s, tiles)
        total = ti * 0
        for b, bit in enumerate(bits):
            if isinstance(s, int):
                total = total + ((1 - bit) if (s >> b) & 1 else bit) * (1 << b)
            else:
                total = total + lax.rem(bit + lax.rem(lax.div(s, 1 << b), 2), 2) * (1 << b)
        return total

    def peer(d):
        if isinstance(d, int):
            s, rest = divmod(d, local)
            p, q = divmod(rest, subs)
        else:
            s, rest = lax.div(d, local), lax.rem(d, local)
            p, q = lax.div(rest, subs), lax.rem(rest, subs)
        t, p, q = tile_at(s), shifted(pi, p, pens), shifted(si, q, subs)
        return {"tile": t, "pen": p, "sub": q}, (t * pens + p) * subs + q

    def each(first, last, body):
        if last - first <= 32:
            for d in range(first, last):
                body(d)
        else:
            def step(d, carry):
                body(d)
                return carry

            lax.fori_loop(first, last, step, 0)

    first_loads = [
        (parts_hbm.at[0, 0], parts_all.at[si]), (bonds_hbm.at[0, 0], bonds_all.at[si]),
        (rest_hbm.at[0, 0], rest_all.at[si]),
        (pos_hbm, pos_in), (vel_hbm, vel_in), (chg_hbm, chg_in), (imass_hbm, imass_in),
        (shown_hbm, shown_in), (offs_hbm, offs_in),
    ]
    later_loads = [
        (mine_hbm.at[:, me], mine_ref), (cas_hbm, cas_ref), (tall_hbm, tall_ref),
        (along_hbm, along_ref), (across_hbm, across_ref), (freq_hbm.at[me], freq_ref),
    ]
    loads = [
        pltpu.make_async_copy(src, dst, load_sem.at[k]) for k, (src, dst) in enumerate(first_loads + later_loads)
    ]
    for copy in loads[: len(first_loads)]:
        copy.start()

    barrier = pltpu.get_barrier_semaphore()
    each(
        1, group,
        lambda d: pl.semaphore_signal(
            barrier, inc=1, device_id=peer(d)[0], device_id_type=pl.DeviceIdType.MESH
        ),
    )
    for copy in loads[len(first_loads) :]:
        copy.start()
    for copy in loads[: len(first_loads)]:
        copy.wait()

    shown = jnp.broadcast_to(shown_in[0], (8, LANES))
    shown_low, shown_high = shown & (LANES - 1), shown >> 7

    def show(blocks):
        total = jnp.zeros((8, LANES), blocks[0].dtype)
        for c, block in enumerate(blocks):
            total = jnp.where(shown_high == c, lane_gather(block, shown_low), total)
        return total

    for c in range(chunks):
        lanes = slice(c * LANES, (c + 1) * LANES)
        rows = [pos_in[r, 0, :, lanes] for r in range(3)] + [chg_in[0, :, lanes]]
        rows += [vel_in[r, 0, :, lanes] for r in range(3)] + [imass_in[0, :, lanes]]
        mine[c] = stacked(rows)
        offset = stacked([offs_in[r, 0, :, lanes].astype(f32) for r in range(3)])
        static_all[patch, :, lanes] = offset[:4]
    mine[shown_chunk] = show([mine[c] for c in range(chunks)])

    def step_copy(n, slot):
        dt, dp = offsets[slot]
        back = offsets.index(((-dt) % tiles, (-dp) % pens))
        device = {"tile": shifted(ti, dt, tiles), "pen": shifted(pi, dp, pens)}
        return remote(sent.at[n], beside.at[n, back], step_send.at[n, slot], step_recv.at[n, back], device)

    def send_shown(n):
        sent[n] = mine[shown_chunk][:4]
        for slot in reversed(range(len(offsets))):
            step_copy(n, slot).start()

    def wait_shown(n):
        for slot in range(len(offsets)):
            remote(
                sent.at[n], beside.at[n, slot], step_send.at[n, slot], step_recv.at[n, slot], {"sub": si}
            ).wait_recv()
            step_copy(n, slot).wait_send()

    def pair_copy(k, source):
        table = (parts_all, bonds_all, rest_all, speeds)[k]
        if k == 3:
            return remote(speeds, speeds, pair_send.at[k, source], pair_recv.at[k, lead], {"sub": source})
        return remote(table.at[source], table.at[source], pair_send.at[k, source], pair_recv.at[k, source], {"sub": lead})

    def static_device(d):
        return {"tile": tile_at(d // pens if isinstance(d, int) else lax.div(d, pens)),
                "pen": shifted(pi, d % pens if isinstance(d, int) else lax.rem(d, pens), pens)}

    def static_copy(d):
        return remote(
            static_all.at[patch], static_all.at[patch], static_send.at[d], static_recv.at[patch], static_device(d)
        )

    pl.semaphore_wait(barrier, group - 1)

    @pl.when(leads)
    def _():
        send_shown(0)

    for source in range(lead):
        @pl.when(si == source)
        def _(source=source):
            for k in range(3):
                pair_copy(k, source).start()

    each(1, tiles * pens, lambda d: static_copy(d).start())

    moves_x, moves_y = [], []
    for i in range(3):
        near = ti + (i - 1)
        moves_x.append(jnp.where(near < 0, -float(GRID), jnp.where(near >= tiles, float(GRID), 0.0)))
        near = pi + (i - 1)
        moves_y.append(jnp.where(near < 0, -float(GRID), jnp.where(near >= pens, float(GRID), 0.0)))

    def work_out(c, g, index):
        high = index >> 7
        block = high
        shx = jnp.zeros((8, LANES), f32)
        shy = jnp.zeros((8, LANES), f32)
        for i in range(3):
            for j in range(3):
                if (i, j) == (1, 1):
                    continue
                hit = high == chunks + i * 3 + j
                step = ((i - 1) % tiles, (j - 1) % pens)
                block = jnp.where(hit, chunks + offsets.index(step), block)
                if i != 1:
                    shx = jnp.where(hit, moves_x[i], shx)
                if j != 1:
                    shy = jnp.where(hit, moves_y[j], shy)
        low_ref[c, g] = index & (LANES - 1)
        blk_ref[c, g] = block
        shx_ref[c, g] = shx
        shy_ref[c, g] = shy

    def set_up():
        for source in range(lead):
            for k in range(3):
                pair_copy(k, source).wait_recv()
        for g in range(groups):
            q, row = divmod(g * 8, slots)
            index = [parts_all[q, row : row + 8, c * LANES : (c + 1) * LANES] for c in range(chunks)]
            for c in everyone:
                work_out(c, g, show(index) if c == shown_chunk else index[c])
        rows_of = [(q, b) for q in range(subs) for b in range(bond_rows)]
        for v in range(bidx_ref.shape[1]):
            part = rows_of[v * 8 : v * 8 + 8]
            numbers, rests = [], []
            for c in range(chunks):
                lanes = slice(c * LANES, (c + 1) * LANES)
                atom = lax.broadcasted_iota(jnp.int32, (1, LANES), 1) + c * LANES
                rows = [bonds_all[q, b : b + 1, lanes] for q, b in part] + [atom] * (8 - len(part))
                numbers.append(stacked(rows))
                rests.append(stacked([rest_all[q, b : b + 1, lanes] for q, b in part]))
                bidx_ref[c, v] = numbers[c]
                brest_ref[c, v] = rests[c]
            bidx_ref[shown_chunk, v] = show(numbers)
            brest_ref[shown_chunk, v] = show(rests)

    def own_tables(rows):
        return [(c, [wide_row(mine[c, r : r + 1, :]) for r in rows]) for c in range(chunks)]

    def around_tables(n, rows):
        return [
            (chunks + slot, [wide_row(beside[n, slot, r : r + 1, :]) for r in rows]) for slot in range(len(offsets))
        ]

    def pick(found, low, block, table):
        for number, sources in table:
            hit = block == number
            found = [jnp.where(hit, lane_gather(source, low), f) for source, f in zip(sources, found)]
        return found

    xyz = (0, 1, 2)

    def near_part():
        table = own_tables(xyz)
        for c in everyone:
            for g in range(groups):
                found = pick([jnp.zeros((8, LANES), f32)] * 3, low_ref[c, g], blk_ref[c, g], table)
                near_ref[c, g, 0] = found[0] + shx_ref[c, g]
                near_ref[c, g, 1] = found[1] + shy_ref[c, g]
                near_ref[c, g, 2] = found[2]
            own = [wide_row(mine[c, r : r + 1, :]) for r in xyz]
            force = [jnp.zeros((8, LANES), f32)] * 3
            for v in range(bidx_ref.shape[1]):
                index = bidx_ref[c, v]
                near = pick([jnp.zeros((8, LANES), f32)] * 3, index & (LANES - 1), index >> 7, table)
                delta = [own[r] - near[r] for r in xyz]
                root = lax.rsqrt(delta[0] * delta[0] + delta[1] * delta[1] + delta[2] * delta[2] + soften)
                pull = -bond_stiffness * (1.0 - brest_ref[c, v] * root)
                force = [force[r] + pull * delta[r] for r in xyz]
            for r in xyz:
                bforce[c, r] = force[r]

    def far_part(n, which):
        table = around_tables(n, xyz)
        for c in which:
            own = [wide_row(mine[c, r : r + 1, :]) for r in xyz]
            force = [bforce[c, r] for r in xyz]
            for g in range(groups):
                shift = (shx_ref[c, g], shy_ref[c, g], 0.0)
                near = [near_ref[c, g, r] for r in xyz]
                low, block = low_ref[c, g], blk_ref[c, g]
                inside = block < chunks
                far = pick([jnp.zeros((8, LANES), f32)] * 3, low, block, table)
                near = [
                    jnp.where(inside, near[r], far[r] if r == 2 else far[r] + shift[r]) for r in xyz
                ]
                delta = [own[r] - near[r] for r in xyz]
                dist_sq = delta[0] * delta[0] + delta[1] * delta[1] + delta[2] * delta[2]
                taper = 1.0 - dist_sq * (1.0 / cutoff_sq)
                taper = jnp.where(dist_sq < cutoff_sq, taper * taper, 0.0)
                root = lax.rsqrt(dist_sq + soften)
                strength = qq_ref[c, g] * taper * (root * root * root)
                force = [force[r] + strength * delta[r] for r in xyz]
            scale = mine[c, 7:8, :]
            for r in xyz:
                total = jnp.sum(force[r], axis=0, keepdims=True)
                speed = mine[c, 4 + r : 5 + r, :] + time_step * scale * total
                mine[c, 4 + r : 5 + r, :] = speed
                mine[c, r : r + 1, :] = mine[c, r : r + 1, :] + time_step * speed

    def charges_once():
        table = own_tables((3,)) + around_tables(0, (3,))
        for c in everyone:
            own = wide_row(mine[c, 3:4, :])
            for g in range(groups):
                (near,) = pick([jnp.zeros((8, LANES), f32)], low_ref[c, g], blk_ref[c, g], table)
                qq_ref[c, g] = coulomb * own * near

    wide_atoms = local * width

    def cells(offset, count):
        return lax.broadcasted_iota(jnp.int32, (count, wide_atoms), 0) - offset

    def row_of(ref, t, r):
        return jnp.concatenate([ref[t * pens + p, r : r + 1, :] for p in range(pens)], axis=1)

    def static_wait(q):
        remote(
            static_all.at[patch], static_all.at[q], static_send.at[0], static_recv.at[q], {"sub": si}
        ).wait_recv()

    def place_wait(q):
        remote(
            pos_all.at[patch], pos_all.at[q], place_send.at[0], place_recv.at[q], {"sub": si}
        ).wait_recv()

    def tile_wait(wait, s, t, own_too):
        for step in range(1, pens):
            wait(t * pens + shifted(pi, step, pens))

        @pl.when(jnp.logical_or(s > 0, own_too))
        def _():
            wait(t * pens + pi)

    def fill(s):
        t = tile_at(s)
        tile_wait(static_wait, s, t, False)
        for r, source, target in ((1, mine_ref, gy), (2, cas_ref, gz)):
            offset = (row_of(static_all, t, r).astype(jnp.int32) + 1) & (GRID - 1)
            hot = jnp.where(cells(offset, GRID) == 0, 1.0, 0.0).astype(bf16)
            rows = source.shape[1]
            part = min(rows, GRID)
            for c in range(0, rows, part):
                value = single(source[0, c : c + part], hot) + single(source[1, c : c + part], hot)
                target[t, c : c + part] = value

    def fill_step(n):
        per = -(-tiles // INNER)
        for k in range(per):
            s = n * per + k
            if tiles % INNER:
                pl.when(s < tiles)(functools.partial(fill, s))
            else:
                fill(s)

    @pl.when(leads)
    def _():
        set_up()

    for copy in loads[len(first_loads) :]:
        copy.wait()

    def clear(j, carry):
        for edge in range(tiles + 1):
            grid[j, edge * planes : edge * planes + 8] = jnp.zeros((8, GRID), f32)
        return carry

    lax.fori_loop(0, share, clear, 0)

    def inner(n, carry):
        @pl.when(leads)
        def _():
            @pl.when(n > 0)
            def _():
                far_part(n - 1, [shown_chunk])
                send_shown(n)
                far_part(n - 1, range(chunks))

            near_part()

        if keep:
            fill_step(n)

        @pl.when(leads)
        def _():
            wait_shown(n)

            @pl.when(n == 0)
            def _():
                charges_once()

        return carry

    lax.fori_loop(0, INNER, inner, 0)

    def place_copy(d):
        return remote(pos_all.at[patch], pos_all.at[patch], place_send.at[d], place_recv.at[patch], peer(d)[0])

    @pl.when(leads)
    def _():
        far_part(INNER - 1, range(chunks))
        for c in range(chunks):
            lanes = slice(c * LANES, (c + 1) * LANES)
            pos_all[patch, :, lanes] = mine[c][:4]
            speeds[:, lanes] = mine[c][4:]
        each(1, group, lambda d: place_copy(d).start())
        for source in range(lead):
            pair_copy(3, source).start()

    if not keep:
        each(1, tiles * pens, lambda d: static_wait(
            static_device(d)["tile"] * pens + static_device(d)["pen"]
        ))
    each(1, tiles * pens, lambda d: static_copy(d).wait_send())
    top = tiles * planes

    def prepare(t, r):
        offset = row_of(static_all, t, r)
        return offset.astype(jnp.int32), row_of(pos_all, t, r) - (offset + 1.0)

    def blend(table, start, count, pieces):
        rows = table.shape[0] // 4
        total = table[start : start + count] * pieces[0]
        for m in range(1, 4):
            total = total + table[m * rows + start : m * rows + start + count] * pieces[m]
        return total

    def depth_of(t):
        offset, frac = prepare(t, 2)
        depth = spline(cells(offset, GRID) & (GRID - 1), frac)
        return split(product((cas_ref[0, GRID : 2 * GRID], cas_ref[1, GRID : 2 * GRID]), split(depth)))

    parts = [(c, min(c + chunk, lows), True) for c in range(0, lows, chunk)]
    parts += [(c, min(c + chunk, share), False) for c in range(lows, share, chunk)]

    def spread(s, carry):
        t = tile_at(s)
        tile_wait(place_wait, s, t, jnp.logical_not(leads))
        offset, frac = prepare(t, 0)
        wx[t] = spline(cells(offset - (t * planes - 1), deep), frac)
        offset, frac = prepare(t, 1)
        if keep:
            wy[t] = blend(gy.at[t], 0, share, spline_pieces(frac))
            pieces = spline_pieces(prepare(t, 2)[1])
            for c in range(0, GRID, 64):
                high, low = split(blend(gz.at[t], c, 64, pieces))
                wz[t, 0, c : c + 64] = high
                wz[t, 1, c : c + 64] = low
            depth = (wz[t, 0], wz[t, 1])
        else:
            rows = spline(cells(offset, GRID) & (GRID - 1), frac)
            wy[t] = product((mine_ref[0, share : 2 * share], mine_ref[1, share : 2 * share]), split(rows))
            depth = depth_of(t)
        wyq[...] = wy[t] * row_of(pos_all, t, 3)
        base = pl.multiple_of(t * planes, 8)
        for start, stop, exact in parts:
            plane = jnp.concatenate([wx[t] * wyq[k : k + 1, :] for k in range(start, stop)], axis=0)
            if exact:
                values = product(split(plane), depth, True)
            else:
                values = single(plane.astype(bf16), depth[0], True)
            values = values.reshape(stop - start, deep, GRID)
            for k in range(start, stop):
                value = values[k - start]
                grid[k, pl.ds(base, 8)] += value[:8]
                if planes > 8:
                    grid[k, pl.ds(pl.multiple_of(base + 8, 8), planes - 8)] = value[8:planes]
                grid[k, pl.ds(pl.multiple_of(base + planes, 8), 8)] += value[planes : planes + 8]
        return carry

    lax.fori_loop(0, tiles, spread, 0)
    for source in range(lead):
        @pl.when(si == source)
        def _(source=source):
            remote(
                speeds, speeds, pair_send.at[3, source], pair_recv.at[3, lead], {"sub": lead}
            ).wait_recv()
    for r in range(3):
        out_ref[r] = pos_all[patch, r : r + 1, :]
        out_ref[3 + r] = speeds[r : r + 1, :]

    def transform(start, stop, exact):
        batch = math.gcd(math.gcd(start, stop), BATCH)

        def step(n, carry):
            first = start + n * batch
            lines = []
            for i in range(batch):
                line = grid[first + i, 0:top]
                edge = line[:8] + grid[first + i, top : top + 8]
                lines.append(jnp.concatenate([edge, line[8:]], axis=0))
            line = split(jnp.concatenate(lines, axis=1))
            spectrum = product((cas_ref[0, :GRID], cas_ref[1, :GRID]), line)
            weighted = []
            for i in range(batch):
                m_sq = along_ref[...] + freq_ref[first + i, 0:1, :]
                anchor = m_sq == 0.0
                value = across_ref[...] * freq_ref[first + i, 1:2, :] / jnp.where(anchor, 1.0, m_sq)
                weighted.append(spectrum[:, i * GRID : (i + 1) * GRID] * jnp.where(anchor, 0.0, value))
            weighted = jnp.concatenate(weighted, axis=1)
            if exact:
                back = product((tall_ref[0], tall_ref[1]), split(weighted))
            else:
                back = half_product((tall_ref[0], tall_ref[1]), weighted.astype(bf16))
            for i in range(batch):
                grid[first + i, 0:top] = back[:, i * GRID : (i + 1) * GRID]
                grid[first + i, top : top + 8] = back[0:8, i * GRID : (i + 1) * GRID]
            return carry

        if stop > start:
            lax.fori_loop(0, (stop - start) // batch, step, 0)

    transform(0, lows, True)
    transform(lows, share, False)

    def part_copy(g, device):
        return remote(part_sent.at[g], part_recv.at[me], part_send_sem.at[g], part_recv_sem.at[me], device)

    def read(n, carry):
        s = tiles - 1 - n
        t = tile_at(s)
        if keep:
            depth = (wz[t, 0], wz[t, 1])
        else:
            depth = depth_of(t)
        base = pl.multiple_of(t * planes, 8)
        total = jnp.zeros((planes + 8, wide_atoms), f32)
        for start, stop, exact in parts:
            rows = [grid[k, pl.ds(base, planes + 8)] for k in range(start, stop)]
            line = jnp.concatenate(rows, axis=0)
            if exact:
                values = product(split(line), depth)
            else:
                values = single(line.astype(bf16), depth[0])
            for k in range(start, stop):
                part = values[(k - start) * (planes + 8) : (k - start + 1) * (planes + 8)]
                total = total + part * wy[t, k : k + 1, :]
        result = jnp.sum(total * wx[t, : planes + 8], axis=0, keepdims=True)
        for q in range(local):
            part_sent[t * local + q] = result[:, q * width : (q + 1) * width]

        def give(p, q):
            device = {"tile": t, "pen": p, "sub": q}
            part_copy((t * pens + p) * subs + q, device).start()

        for d in range(1, local):
            give(shifted(pi, d // subs, pens), shifted(si, d % subs, subs))

        @pl.when(s > 0)
        def _():
            give(pi, si)

        return carry

    lax.fori_loop(0, tiles, read, 0)
    part_recv[me] = part_sent[me]

    @pl.when(leads)
    def _():
        each(1, group, lambda d: place_copy(d).wait_send())
        for source in range(lead):
            pair_copy(3, source).wait_send()

    for source in range(lead):
        @pl.when(si == source)
        def _(source=source):
            for k in range(3):
                pair_copy(k, source).wait_send()

    def finish(d):
        device, g = peer(d)
        part_copy(g, device).wait_send()
        remote(part_sent.at[me], part_recv.at[g], part_send_sem.at[g], part_recv_sem.at[g], {"sub": si}).wait_recv()

    each(1, group, finish)
    out_ref[6, :, 0:width] = jnp.sum(part_recv[...], axis=0)
    out_ref[6, :, width:] = jnp.zeros((1, atoms - width), f32)


def halves(table):
    table = jnp.asarray(table.astype(np.float32))
    return jnp.stack(split(table))


def tables(group, shifts):
    share = GRID // group
    index = np.arange(GRID)
    angle = 2.0 * math.pi / GRID * np.mod(index[:, None] * index[None, :], GRID)
    cas = np.cos(angle) + np.sin(angle)
    order = np.array([(r + 1) // 2 if r % 2 else (GRID - r // 2) % GRID for r in range(GRID)])
    dealt = order.reshape(share, group).T
    signed = np.where(index > GRID // 2, index - GRID, index).astype(np.float64)
    turn = 2.0 * math.pi / GRID * index
    real = (1.0 + 4.0 * np.cos(turn) + np.cos(2.0 * turn)) / 6.0
    imag = (4.0 * np.sin(turn) + np.sin(2.0 * turn)) / 6.0
    square = signed**2 / float(GRID * GRID)
    line = np.exp(-((math.pi / ewald_beta) ** 2) * square) / (real * real + imag * imag)
    along = square[:, None] + square[None, :]
    across = line[:, None] * line[None, :] / (math.pi * float(GRID) ** 3)
    flat = dealt.reshape(-1)
    shifted = [cas[:, np.mod(index + m, GRID)] for m in range(-1, shifts - 1)]
    return (
        np.concatenate(shifted), shifted[0].T, np.concatenate([cells[dealt] for cells in shifted], axis=1), line[flat].astype(np.float32), square[flat].astype(np.float32),
        along.astype(np.float32), across.astype(np.float32),
    )


def on_device(
    positions, velocities, charges, inverse_mass, export_rows, partners, bond_partners, bond_rest, block_offsets,
):
    tiles, pens, subs = lax.axis_size("tile"), lax.axis_size("pen"), lax.axis_size("sub")
    local = pens * subs
    group = tiles * local
    atoms, exported = positions.shape[3], export_rows.shape[2]
    slots, bond_rows = partners.shape[2], bond_partners.shape[2]
    width = atoms // subs
    chunks = atoms // LANES
    groups = subs * slots // 8
    planes = GRID // tiles
    share = GRID // group
    lows = min(share, max(1, -(-LOW // group)))
    chunk = math.gcd(share, 8)
    unit = 8 if chunk % 2 == 0 else 16
    deep = -(-(planes + 8) // unit) * unit
    wide_atoms = local * width
    keep = group * width * GRID * 4 <= 16 * 1024 * 1024
    cas, tall, dealt, line, square, along, across = tables(group, 4 if keep else 2)
    around = {((i - 1) % tiles, (j - 1) % pens) for i in range(3) for j in range(3)} - {(0, 0)}
    near = len(around)
    bond_tiles = -(-subs * bond_rows // 8)
    assert exported == LANES and slots % 8 == 0 and planes % 8 == 0
    hbm = pl.BlockSpec(memory_space=pltpu.HBM)
    i32 = jnp.int32
    dma = pltpu.SemaphoreType.DMA

    def vmem(shape, kind=f32):
        return pltpu.VMEM(shape, kind)

    loaded = (
        positions, velocities, charges, inverse_mass, export_rows, partners, bond_partners, bond_rest, block_offsets,
    )
    freq = np.broadcast_to(np.stack([square, line], axis=1).reshape(group, share, 2, 1), (group, share, 2, GRID))
    constants = (
        halves(dealt), halves(cas), halves(tall), jnp.asarray(along), jnp.asarray(across), jnp.asarray(freq),
    )
    tile = (8, LANES)
    patches = tiles * pens
    scratch = [vmem(x.shape, x.dtype) for x in loaded]
    scratch[5:8] = [
        vmem((subs, slots, atoms), i32), vmem((subs, bond_rows, atoms), i32), vmem((subs, bond_rows, atoms)),
    ]
    kernel = functools.partial(
        program_kernel, tiles=tiles, pens=pens, subs=subs, planes=planes, deep=deep, share=share, lows=lows,
        chunk=chunk, keep=keep,
    )
    out = pl.pallas_call(
        kernel,
        out_shape=jax.ShapeDtypeStruct((7, 1, atoms), f32),
        in_specs=[hbm] * (len(loaded) + len(constants)),
        out_specs=pl.BlockSpec(memory_space=pltpu.VMEM),
        scratch_shapes=scratch
        + [vmem((2, dealt.shape[1], GRID), bf16)]
        + [vmem(x.shape, x.dtype) for x in constants[1:5]]
        + [
            vmem((share, 2, GRID)),
            vmem((chunks + 1,) + tile), vmem((INNER, 4, LANES)), vmem((INNER, near, 4, LANES)),
            vmem((patches, 4, atoms)), vmem((patches, 4, atoms)), vmem((4, atoms)),
            vmem((chunks + 1, groups) + tile, i32), vmem((chunks + 1, groups) + tile, i32),
            vmem((chunks + 1, groups) + tile), vmem((chunks + 1, groups) + tile), vmem((chunks + 1, groups) + tile),
            vmem((chunks + 1, groups, 3) + tile), vmem((chunks + 1, 3) + tile),
            vmem((chunks + 1, bond_tiles) + tile, i32), vmem((chunks + 1, bond_tiles) + tile),
            vmem((share, GRID + 8, GRID)), vmem((tiles, deep, wide_atoms)), vmem((tiles, share, wide_atoms)),
            vmem((share, wide_atoms)), vmem((tiles if keep else 1, 2, GRID, wide_atoms), bf16),
            vmem((tiles, 4 * GRID, wide_atoms) if keep else (1, 8, LANES)),
            vmem((tiles, 4 * share, wide_atoms) if keep else (1, 8, LANES)),
            vmem((group, 1, width)), vmem((group, 1, width)),
            dma((15,)), dma((INNER, near)), dma((INNER, near)), dma((4, subs)), dma((4, subs)),
            dma((patches,)), dma((patches,)), dma((group,)), dma((patches,)), dma((group,)), dma((group,)),
        ],
        compiler_params=pltpu.CompilerParams(
            collective_id=0, has_side_effects=True, vmem_limit_bytes=VMEM_LIMIT
        ),
    )(*loaded, *constants)
    return out[0:3].reshape(positions.shape), out[3:6].reshape(velocities.shape), out[6:7, :, :width]


def solution(mesh):
    placed = (
        P("rep", "tile", "pen", None),
        P("rep", "tile", "pen", None),
        P(("rep", "tile"), "pen", None),
        P(("rep", "tile"), "pen", None),
        P(("rep", "tile"), "pen", None),
        P(("rep", "tile"), "pen", "sub", None),
        P(("rep", "tile"), "pen", "sub", None),
        P(("rep", "tile"), "pen", "sub", None),
        P("rep", "tile", "pen", None),
    )
    return jax.shard_map(
        on_device,
        mesh=mesh,
        in_specs=placed,
        out_specs=(
            P("rep", "tile", "pen", None),
            P("rep", "tile", "pen", None),
            P(("rep", "tile"), "pen", "sub"),
        ),
        check_vma=False,
    )
```

```python
import functools
import math

import jax
import jax.numpy as jnp
import numpy as np
from jax import lax
from jax.experimental import pallas as pl
from jax.experimental.pallas import tpu as pltpu
from jax.sharding import PartitionSpec as P

GRID = 256
INNER = 4
LANES = 128
LOW = 128
BATCH = 8
VMEM_LIMIT = 60 * 1024 * 1024

time_step = 0.1
coulomb = 30.0
bond_stiffness = 0.2
soften = 1.0
cutoff_sq = 144.0
ewald_beta = 0.32

f32 = jnp.float32
bf16 = jnp.bfloat16


def lane_gather(rows, low):
    return jnp.take_along_axis(rows, low, axis=1, mode="promise_in_bounds")


def split(value):
    high = value.astype(bf16)
    return high, (value - high.astype(f32)).astype(bf16)


def single(left, right, turned=False):
    dims = (((1,), (1 if turned else 0,)), ((), ()))
    return lax.dot_general(left, right, dims, preferred_element_type=f32)


def product(left, right, turned=False):
    return single(left[0], right[0], turned) + (
        single(left[0], right[1], turned) + single(left[1], right[0], turned)
    )


def half_product(left, right, turned=False):
    return single(left[0], right, turned) + single(left[1], right, turned)


def spline_pieces(frac):
    rest = 1.0 - frac
    square = frac * frac
    cube = square * frac
    sixth = 1.0 / 6.0
    return (
        rest * rest * rest * sixth,
        (3.0 * cube - 6.0 * square + 4.0) * sixth,
        (-3.0 * cube + 3.0 * square + 3.0 * frac + 1.0) * sixth,
        cube * sixth,
    )


def spline(place, frac):
    pieces = spline_pieces(frac)
    total = jnp.zeros(place.shape, f32)
    for order in range(4):
        total = jnp.where(place == order, pieces[order], total)
    return total


def wide_row(row):
    return jnp.broadcast_to(row, (8, LANES))


def stacked(rows):
    place = lax.broadcasted_iota(jnp.int32, (8, LANES), 0)
    total = jnp.zeros((8, LANES), rows[0].dtype)
    for r, row in enumerate(rows):
        total = jnp.where(place == r, wide_row(row), total)
    return total


def program_kernel(
    pos_hbm, vel_hbm, chg_hbm, imass_hbm, shown_hbm, parts_hbm, bonds_hbm, rest_hbm, offs_hbm,
    mine_hbm, cas_hbm, tall_hbm, along_hbm, across_hbm, freq_hbm,
    out_ref,
    pos_in, vel_in, chg_in, imass_in, shown_in, parts_all, bonds_all, rest_all, offs_in,
    mine_ref, cas_ref, tall_ref, along_ref, across_ref, freq_ref,
    mine, sent, beside, static_all, pos_all, speeds,
    low_ref, blk_ref, shx_ref, shy_ref, qq_ref, near_ref, bforce, bidx_ref, brest_ref,
    grid, wx, wy, wyq, wz, gz, gy, part_sent, part_recv,
    load_sem, step_send, step_recv, pair_send, pair_recv,
    static_send, static_recv, place_send, place_recv, part_send_sem, part_recv_sem,
    *, tiles, pens, subs, planes, deep, share, lows, chunk, keep,
):
    ti, pi, si = lax.axis_index("tile"), lax.axis_index("pen"), lax.axis_index("sub")
    lead = subs - 1
    leads = si == lead
    local = pens * subs
    group = tiles * local
    patch = ti * pens + pi
    me = patch * subs + si
    atoms = pos_in.shape[3]
    width = atoms // subs
    chunks = atoms // LANES
    shown_chunk = chunks
    slots = parts_all.shape[1]
    groups = subs * slots // 8
    bond_rows = bonds_all.shape[1]
    everyone = range(chunks + 1)

    offsets = []
    for i in range(3):
        for j in range(3):
            step = ((i - 1) % tiles, (j - 1) % pens)
            if step != (0, 0) and step not in offsets:
                offsets.append(step)

    def remote(src, dst, send, recv, device):
        return pltpu.make_async_remote_copy(
            src_ref=src, dst_ref=dst, send_sem=send, recv_sem=recv,
            device_id=device, device_id_type=pl.DeviceIdType.MESH,
        )

    def shifted(index, step, count):
        if isinstance(step, int):
            moved = index + step % count
            return moved if step % count == 0 else jnp.where(moved >= count, moved - count, moved)
        return lax.rem(index + step, count)

    bits = []
    if tiles & (tiles - 1) == 0:
        bits = [lax.rem(lax.div(ti, 1 << b), 2) for b in range(tiles.bit_length() - 1)]

    def tile_at(s):
        if tiles & (tiles - 1):
            return shifted(ti, s, tiles)
        total = ti * 0
        for b, bit in enumerate(bits):
            if isinstance(s, int):
                total = total + ((1 - bit) if (s >> b) & 1 else bit) * (1 << b)
            else:
                total = total + lax.rem(bit + lax.rem(lax.div(s, 1 << b), 2), 2) * (1 << b)
        return total

    def peer(d):
        if isinstance(d, int):
            s, rest = divmod(d, local)
            p, q = divmod(rest, subs)
        else:
            s, rest = lax.div(d, local), lax.rem(d, local)
            p, q = lax.div(rest, subs), lax.rem(rest, subs)
        t, p, q = tile_at(s), shifted(pi, p, pens), shifted(si, q, subs)
        return {"tile": t, "pen": p, "sub": q}, (t * pens + p) * subs + q

    def each(first, last, body):
        if last - first <= 32:
            for d in range(first, last):
                body(d)
        else:
            def step(d, carry):
                body(d)
                return carry

            lax.fori_loop(first, last, step, 0)

    first_loads = [
        (parts_hbm.at[0, 0], parts_all.at[si]), (bonds_hbm.at[0, 0], bonds_all.at[si]),
        (rest_hbm.at[0, 0], rest_all.at[si]),
        (pos_hbm, pos_in), (vel_hbm, vel_in), (chg_hbm, chg_in), (imass_hbm, imass_in),
        (shown_hbm, shown_in), (offs_hbm, offs_in),
    ]
    later_loads = [
        (mine_hbm.at[:, me], mine_ref), (cas_hbm, cas_ref), (tall_hbm, tall_ref),
        (along_hbm, along_ref), (across_hbm, across_ref), (freq_hbm.at[me], freq_ref),
    ]
    loads = [
        pltpu.make_async_copy(src, dst, load_sem.at[k]) for k, (src, dst) in enumerate(first_loads + later_loads)
    ]
    for copy in loads[: len(first_loads)]:
        copy.start()

    barrier = pltpu.get_barrier_semaphore()
    each(
        1, group,
        lambda d: pl.semaphore_signal(
            barrier, inc=1, device_id=peer(d)[0], device_id_type=pl.DeviceIdType.MESH
        ),
    )
    for copy in loads[len(first_loads) :]:
        copy.start()
    for copy in loads[: len(first_loads)]:
        copy.wait()

    shown = jnp.broadcast_to(shown_in[0], (8, LANES))
    shown_low, shown_high = shown & (LANES - 1), shown >> 7

    def show(blocks):
        total = jnp.zeros((8, LANES), blocks[0].dtype)
        for c, block in enumerate(blocks):
            total = jnp.where(shown_high == c, lane_gather(block, shown_low), total)
        return total

    for c in range(chunks):
        lanes = slice(c * LANES, (c + 1) * LANES)
        rows = [pos_in[r, 0, :, lanes] for r in range(3)] + [chg_in[0, :, lanes]]
        rows += [vel_in[r, 0, :, lanes] for r in range(3)] + [imass_in[0, :, lanes]]
        mine[c] = stacked(rows)
        offset = stacked([offs_in[r, 0, :, lanes].astype(f32) for r in range(3)])
        static_all[patch, :, lanes] = offset[:4]
    mine[shown_chunk] = show([mine[c] for c in range(chunks)])

    def step_copy(n, slot):
        dt, dp = offsets[slot]
        back = offsets.index(((-dt) % tiles, (-dp) % pens))
        device = {"tile": shifted(ti, dt, tiles), "pen": shifted(pi, dp, pens)}
        return remote(sent.at[n], beside.at[n, back], step_send.at[n, slot], step_recv.at[n, back], device)

    def send_shown(n):
        sent[n] = mine[shown_chunk][:4]
        for slot in reversed(range(len(offsets))):
            step_copy(n, slot).start()

    def wait_shown(n):
        for slot in range(len(offsets)):
            remote(
                sent.at[n], beside.at[n, slot], step_send.at[n, slot], step_recv.at[n, slot], {"sub": si}
            ).wait_recv()
            step_copy(n, slot).wait_send()

    def pair_copy(k, source):
        table = (parts_all, bonds_all, rest_all, speeds)[k]
        if k == 3:
            return remote(speeds, speeds, pair_send.at[k, source], pair_recv.at[k, lead], {"sub": source})
        return remote(table.at[source], table.at[source], pair_send.at[k, source], pair_recv.at[k, source], {"sub": lead})

    def static_device(d):
        return {"tile": tile_at(d // pens if isinstance(d, int) else lax.div(d, pens)),
                "pen": shifted(pi, d % pens if isinstance(d, int) else lax.rem(d, pens), pens)}

    def static_copy(d):
        return remote(
            static_all.at[patch], static_all.at[patch], static_send.at[d], static_recv.at[patch], static_device(d)
        )

    moves_x, moves_y = [], []
    for i in range(3):
        near = ti + (i - 1)
        moves_x.append(jnp.where(near < 0, -float(GRID), jnp.where(near >= tiles, float(GRID), 0.0)))
        near = pi + (i - 1)
        moves_y.append(jnp.where(near < 0, -float(GRID), jnp.where(near >= pens, float(GRID), 0.0)))

    def work_out(c, g, index):
        high = index >> 7
        block = high
        shx = jnp.zeros((8, LANES), f32)
        shy = jnp.zeros((8, LANES), f32)
        for i in range(3):
            for j in range(3):
                if (i, j) == (1, 1):
                    continue
                hit = high == chunks + i * 3 + j
                step = ((i - 1) % tiles, (j - 1) % pens)
                block = jnp.where(hit, chunks + offsets.index(step), block)
                if i != 1:
                    shx = jnp.where(hit, moves_x[i], shx)
                if j != 1:
                    shy = jnp.where(hit, moves_y[j], shy)
        low_ref[c, g] = index & (LANES - 1)
        blk_ref[c, g] = block
        shx_ref[c, g] = shx
        shy_ref[c, g] = shy

    def set_up_rows(some):
        for g in range(groups):
            q, row = divmod(g * 8, slots)
            if q not in some:
                continue
            index = [parts_all[q, row : row + 8, c * LANES : (c + 1) * LANES] for c in range(chunks)]
            for c in everyone:
                work_out(c, g, show(index) if c == shown_chunk else index[c])

    def set_up():
        for source in range(lead):
            for k in range(3):
                pair_copy(k, source).wait_recv()
        set_up_rows(range(lead))
        rows_of = [(q, b) for q in range(subs) for b in range(bond_rows)]
        for v in range(bidx_ref.shape[1]):
            part = rows_of[v * 8 : v * 8 + 8]
            numbers, rests = [], []
            for c in range(chunks):
                lanes = slice(c * LANES, (c + 1) * LANES)
                atom = lax.broadcasted_iota(jnp.int32, (1, LANES), 1) + c * LANES
                rows = [bonds_all[q, b : b + 1, lanes] for q, b in part] + [atom] * (8 - len(part))
                numbers.append(stacked(rows))
                rests.append(stacked([rest_all[q, b : b + 1, lanes] for q, b in part]))
                bidx_ref[c, v] = numbers[c]
                brest_ref[c, v] = rests[c]
            bidx_ref[shown_chunk, v] = show(numbers)
            brest_ref[shown_chunk, v] = show(rests)

    def own_tables(rows):
        return [(c, [wide_row(mine[c, r : r + 1, :]) for r in rows]) for c in range(chunks)]

    def around_tables(n, rows):
        return [
            (chunks + slot, [wide_row(beside[n, slot, r : r + 1, :]) for r in rows]) for slot in range(len(offsets))
        ]

    def pick(found, low, block, table):
        for number, sources in table:
            hit = block == number
            found = [jnp.where(hit, lane_gather(source, low), f) for source, f in zip(sources, found)]
        return found

    xyz = (0, 1, 2)

    def near_part():
        table = own_tables(xyz)
        for c in everyone:
            for g in range(groups):
                found = pick([jnp.zeros((8, LANES), f32)] * 3, low_ref[c, g], blk_ref[c, g], table)
                near_ref[c, g, 0] = found[0] + shx_ref[c, g]
                near_ref[c, g, 1] = found[1] + shy_ref[c, g]
                near_ref[c, g, 2] = found[2]
            own = [wide_row(mine[c, r : r + 1, :]) for r in xyz]
            force = [jnp.zeros((8, LANES), f32)] * 3
            for v in range(bidx_ref.shape[1]):
                index = bidx_ref[c, v]
                near = pick([jnp.zeros((8, LANES), f32)] * 3, index & (LANES - 1), index >> 7, table)
                delta = [own[r] - near[r] for r in xyz]
                root = lax.rsqrt(delta[0] * delta[0] + delta[1] * delta[1] + delta[2] * delta[2] + soften)
                pull = -bond_stiffness * (1.0 - brest_ref[c, v] * root)
                force = [force[r] + pull * delta[r] for r in xyz]
            for r in xyz:
                bforce[c, r] = force[r]

    def far_part(n, which):
        table = around_tables(n, xyz)
        for c in which:
            own = [wide_row(mine[c, r : r + 1, :]) for r in xyz]
            force = [bforce[c, r] for r in xyz]
            for g in range(groups):
                shift = (shx_ref[c, g], shy_ref[c, g], 0.0)
                near = [near_ref[c, g, r] for r in xyz]
                low, block = low_ref[c, g], blk_ref[c, g]
                inside = block < chunks
                far = pick([jnp.zeros((8, LANES), f32)] * 3, low, block, table)
                near = [
                    jnp.where(inside, near[r], far[r] if r == 2 else far[r] + shift[r]) for r in xyz
                ]
                delta = [own[r] - near[r] for r in xyz]
                dist_sq = delta[0] * delta[0] + delta[1] * delta[1] + delta[2] * delta[2]
                taper = 1.0 - dist_sq * (1.0 / cutoff_sq)
                taper = jnp.where(dist_sq < cutoff_sq, taper * taper, 0.0)
                root = lax.rsqrt(dist_sq + soften)
                strength = qq_ref[c, g] * taper * (root * root * root)
                force = [force[r] + strength * delta[r] for r in xyz]
            scale = mine[c, 7:8, :]
            for r in xyz:
                total = jnp.sum(force[r], axis=0, keepdims=True)
                speed = mine[c, 4 + r : 5 + r, :] + time_step * scale * total
                mine[c, 4 + r : 5 + r, :] = speed
                mine[c, r : r + 1, :] = mine[c, r : r + 1, :] + time_step * speed

    def charges_once():
        table = own_tables((3,)) + around_tables(0, (3,))
        for c in everyone:
            own = wide_row(mine[c, 3:4, :])
            for g in range(groups):
                (near,) = pick([jnp.zeros((8, LANES), f32)], low_ref[c, g], blk_ref[c, g], table)
                qq_ref[c, g] = coulomb * own * near

    wide_atoms = local * width

    def cells(offset, count):
        return lax.broadcasted_iota(jnp.int32, (count, wide_atoms), 0) - offset

    def row_of(ref, t, r):
        return jnp.concatenate([ref[t * pens + p, r : r + 1, :] for p in range(pens)], axis=1)

    def static_wait(q):
        remote(
            static_all.at[patch], static_all.at[q], static_send.at[0], static_recv.at[q], {"sub": si}
        ).wait_recv()

    def place_wait(q):
        remote(
            pos_all.at[patch], pos_all.at[q], place_send.at[0], place_recv.at[q], {"sub": si}
        ).wait_recv()

    def tile_wait(wait, s, t, own_too):
        for step in range(1, pens):
            wait(t * pens + shifted(pi, step, pens))

        @pl.when(jnp.logical_or(s > 0, own_too))
        def _():
            wait(t * pens + pi)

    def fill(s):
        t = tile_at(s)
        tile_wait(static_wait, s, t, False)
        for r, source, target in ((1, mine_ref, gy), (2, cas_ref, gz)):
            offset = (row_of(static_all, t, r).astype(jnp.int32) + 1) & (GRID - 1)
            hot = jnp.where(cells(offset, GRID) == 0, 1.0, 0.0).astype(bf16)
            rows = source.shape[1]
            part = min(rows, GRID)
            for c in range(0, rows, part):
                value = single(source[0, c : c + part], hot) + single(source[1, c : c + part], hot)
                target[t, c : c + part] = value

    def fill_step(n):
        per = -(-tiles // INNER)
        for k in range(per):
            s = n * per + k
            if tiles % INNER:
                pl.when(s < tiles)(functools.partial(fill, s))
            else:
                fill(s)

    pl.when(leads)(functools.partial(set_up_rows, [lead]))
    pl.semaphore_wait(barrier, group - 1)

    @pl.when(leads)
    def _():
        send_shown(0)

    for source in range(lead):
        @pl.when(si == source)
        def _(source=source):
            for k in range(3):
                pair_copy(k, source).start()

    each(1, tiles * pens, lambda d: static_copy(d).start())

    @pl.when(leads)
    def _():
        set_up()

    for copy in loads[len(first_loads) :]:
        copy.wait()

    def clear(j, carry):
        for edge in range(tiles + 1):
            grid[j, edge * planes : edge * planes + 8] = jnp.zeros((8, GRID), f32)
        return carry

    lax.fori_loop(0, share, clear, 0)

    def inner(n, carry):
        @pl.when(leads)
        def _():
            @pl.when(n > 0)
            def _():
                far_part(n - 1, [shown_chunk])
                send_shown(n)
                far_part(n - 1, range(chunks))

            near_part()

        if keep:
            fill_step(n)

        @pl.when(leads)
        def _():
            wait_shown(n)

            @pl.when(n == 0)
            def _():
                charges_once()

        return carry

    lax.fori_loop(0, INNER, inner, 0)

    def place_copy(d):
        return remote(pos_all.at[patch], pos_all.at[patch], place_send.at[d], place_recv.at[patch], peer(d)[0])

    @pl.when(leads)
    def _():
        far_part(INNER - 1, range(chunks))
        for c in range(chunks):
            lanes = slice(c * LANES, (c + 1) * LANES)
            pos_all[patch, :, lanes] = mine[c][:4]
            speeds[:, lanes] = mine[c][4:]
        each(1, group, lambda d: place_copy(d).start())
        for source in range(lead):
            pair_copy(3, source).start()

    if not keep:
        each(1, tiles * pens, lambda d: static_wait(
            static_device(d)["tile"] * pens + static_device(d)["pen"]
        ))
    each(1, tiles * pens, lambda d: static_copy(d).wait_send())
    top = tiles * planes

    def prepare(t, r):
        offset = row_of(static_all, t, r)
        return offset.astype(jnp.int32), row_of(pos_all, t, r) - (offset + 1.0)

    def blend(table, start, count, pieces):
        rows = table.shape[0] // 4
        total = table[start : start + count] * pieces[0]
        for m in range(1, 4):
            total = total + table[m * rows + start : m * rows + start + count] * pieces[m]
        return total

    def depth_of(t):
        offset, frac = prepare(t, 2)
        depth = spline(cells(offset, GRID) & (GRID - 1), frac)
        return split(product((cas_ref[0, GRID : 2 * GRID], cas_ref[1, GRID : 2 * GRID]), split(depth)))

    parts = [(c, min(c + chunk, lows), True) for c in range(0, lows, chunk)]
    parts += [(c, min(c + chunk, share), False) for c in range(lows, share, chunk)]

    def spread(s, carry):
        t = tile_at(s)
        tile_wait(place_wait, s, t, jnp.logical_not(leads))
        offset, frac = prepare(t, 0)
        wx[t] = spline(cells(offset - (t * planes - 1), deep), frac)
        offset, frac = prepare(t, 1)
        if keep:
            wy[t] = blend(gy.at[t], 0, share, spline_pieces(frac))
            pieces = spline_pieces(prepare(t, 2)[1])
            for c in range(0, GRID, 64):
                high, low = split(blend(gz.at[t], c, 64, pieces))
                wz[t, 0, c : c + 64] = high
                wz[t, 1, c : c + 64] = low
            depth = (wz[t, 0], wz[t, 1])
        else:
            rows = spline(cells(offset, GRID) & (GRID - 1), frac)
            wy[t] = product((mine_ref[0, share : 2 * share], mine_ref[1, share : 2 * share]), split(rows))
            depth = depth_of(t)
        wyq[...] = wy[t] * row_of(pos_all, t, 3)
        base = pl.multiple_of(t * planes, 8)
        for start, stop, exact in parts:
            plane = jnp.concatenate([wx[t] * wyq[k : k + 1, :] for k in range(start, stop)], axis=0)
            if exact:
                values = product(split(plane), depth, True)
            else:
                values = single(plane.astype(bf16), depth[0], True)
            values = values.reshape(stop - start, deep, GRID)
            for k in range(start, stop):
                value = values[k - start]
                grid[k, pl.ds(base, 8)] += value[:8]
                if planes > 8:
                    grid[k, pl.ds(pl.multiple_of(base + 8, 8), planes - 8)] = value[8:planes]
                grid[k, pl.ds(pl.multiple_of(base + planes, 8), 8)] += value[planes : planes + 8]
        return carry

    lax.fori_loop(0, tiles, spread, 0)
    for source in range(lead):
        @pl.when(si == source)
        def _(source=source):
            remote(
                speeds, speeds, pair_send.at[3, source], pair_recv.at[3, lead], {"sub": lead}
            ).wait_recv()
    for r in range(3):
        out_ref[r] = pos_all[patch, r : r + 1, :]
        out_ref[3 + r] = speeds[r : r + 1, :]

    def transform(start, stop, exact):
        batch = math.gcd(math.gcd(start, stop), BATCH)

        def step(n, carry):
            first = start + n * batch
            lines = []
            for i in range(batch):
                line = grid[first + i, 0:top]
                edge = line[:8] + grid[first + i, top : top + 8]
                lines.append(jnp.concatenate([edge, line[8:]], axis=0))
            line = split(jnp.concatenate(lines, axis=1))
            spectrum = product((cas_ref[0, :GRID], cas_ref[1, :GRID]), line)
            weighted = []
            for i in range(batch):
                m_sq = along_ref[...] + freq_ref[first + i, 0:1, :]
                anchor = m_sq == 0.0
                value = across_ref[...] * freq_ref[first + i, 1:2, :] / jnp.where(anchor, 1.0, m_sq)
                weighted.append(spectrum[:, i * GRID : (i + 1) * GRID] * jnp.where(anchor, 0.0, value))
            weighted = jnp.concatenate(weighted, axis=1)
            if exact:
                back = product((tall_ref[0], tall_ref[1]), split(weighted))
            else:
                back = half_product((tall_ref[0], tall_ref[1]), weighted.astype(bf16))
            for i in range(batch):
                grid[first + i, 0:top] = back[:, i * GRID : (i + 1) * GRID]
                grid[first + i, top : top + 8] = back[0:8, i * GRID : (i + 1) * GRID]
            return carry

        if stop > start:
            lax.fori_loop(0, (stop - start) // batch, step, 0)

    transform(0, lows, True)
    transform(lows, share, False)

    def part_copy(g, device):
        return remote(part_sent.at[g], part_recv.at[me], part_send_sem.at[g], part_recv_sem.at[me], device)

    def read(n, carry):
        s = tiles - 1 - n
        t = tile_at(s)
        if keep:
            depth = (wz[t, 0], wz[t, 1])
        else:
            depth = depth_of(t)
        base = pl.multiple_of(t * planes, 8)
        total = jnp.zeros((planes + 8, wide_atoms), f32)
        for start, stop, exact in parts:
            rows = [grid[k, pl.ds(base, planes + 8)] for k in range(start, stop)]
            line = jnp.concatenate(rows, axis=0)
            if exact:
                values = product(split(line), depth)
            else:
                values = single(line.astype(bf16), depth[0])
            for k in range(start, stop):
                part = values[(k - start) * (planes + 8) : (k - start + 1) * (planes + 8)]
                total = total + part * wy[t, k : k + 1, :]
        result = jnp.sum(total * wx[t, : planes + 8], axis=0, keepdims=True)
        for q in range(local):
            part_sent[t * local + q] = result[:, q * width : (q + 1) * width]

        def give(p, q):
            device = {"tile": t, "pen": p, "sub": q}
            part_copy((t * pens + p) * subs + q, device).start()

        for d in range(1, local):
            give(shifted(pi, d // subs, pens), shifted(si, d % subs, subs))

        @pl.when(s > 0)
        def _():
            give(pi, si)

        return carry

    lax.fori_loop(0, tiles, read, 0)
    part_recv[me] = part_sent[me]

    @pl.when(leads)
    def _():
        each(1, group, lambda d: place_copy(d).wait_send())
        for source in range(lead):
            pair_copy(3, source).wait_send()

    for source in range(lead):
        @pl.when(si == source)
        def _(source=source):
            for k in range(3):
                pair_copy(k, source).wait_send()

    def finish(d):
        device, g = peer(d)
        part_copy(g, device).wait_send()
        remote(part_sent.at[me], part_recv.at[g], part_send_sem.at[g], part_recv_sem.at[g], {"sub": si}).wait_recv()

    each(1, group, finish)
    out_ref[6, :, 0:width] = jnp.sum(part_recv[...], axis=0)
    out_ref[6, :, width:] = jnp.zeros((1, atoms - width), f32)


def halves(table):
    table = jnp.asarray(table.astype(np.float32))
    return jnp.stack(split(table))


def tables(group, shifts):
    share = GRID // group
    index = np.arange(GRID)
    angle = 2.0 * math.pi / GRID * np.mod(index[:, None] * index[None, :], GRID)
    cas = np.cos(angle) + np.sin(angle)
    order = np.array([(r + 1) // 2 if r % 2 else (GRID - r // 2) % GRID for r in range(GRID)])
    dealt = order.reshape(share, group).T
    signed = np.where(index > GRID // 2, index - GRID, index).astype(np.float64)
    turn = 2.0 * math.pi / GRID * index
    real = (1.0 + 4.0 * np.cos(turn) + np.cos(2.0 * turn)) / 6.0
    imag = (4.0 * np.sin(turn) + np.sin(2.0 * turn)) / 6.0
    square = signed**2 / float(GRID * GRID)
    line = np.exp(-((math.pi / ewald_beta) ** 2) * square) / (real * real + imag * imag)
    along = square[:, None] + 0.5 * square[None, :]
    across = line[:, None] * np.sqrt(line)[None, :] / (math.pi * float(GRID) ** 3)
    freq = np.stack(
        [square[dealt][..., None] + 0.5 * square, line[dealt][..., None] * np.sqrt(line)], axis=2
    )
    shifted = [cas[:, np.mod(index + m, GRID)] for m in range(-1, shifts - 1)]
    return (
        np.concatenate(shifted), shifted[0].T, np.concatenate([cells[dealt] for cells in shifted], axis=1),
        freq.astype(np.float32), along.astype(np.float32), across.astype(np.float32),
    )


def on_device(
    positions, velocities, charges, inverse_mass, export_rows, partners, bond_partners, bond_rest, block_offsets,
):
    tiles, pens, subs = lax.axis_size("tile"), lax.axis_size("pen"), lax.axis_size("sub")
    local = pens * subs
    group = tiles * local
    atoms, exported = positions.shape[3], export_rows.shape[2]
    slots, bond_rows = partners.shape[2], bond_partners.shape[2]
    width = atoms // subs
    chunks = atoms // LANES
    groups = subs * slots // 8
    planes = GRID // tiles
    share = GRID // group
    lows = min(share, max(1, -(-LOW // group)))
    chunk = math.gcd(share, 8)
    unit = 8 if chunk % 2 == 0 else 16
    deep = -(-(planes + 8) // unit) * unit
    wide_atoms = local * width
    keep = group * width * GRID * 4 <= 16 * 1024 * 1024
    cas, tall, dealt, freq, along, across = tables(group, 4 if keep else 2)
    around = {((i - 1) % tiles, (j - 1) % pens) for i in range(3) for j in range(3)} - {(0, 0)}
    near = len(around)
    bond_tiles = -(-subs * bond_rows // 8)
    assert exported == LANES and slots % 8 == 0 and planes % 8 == 0
    hbm = pl.BlockSpec(memory_space=pltpu.HBM)
    i32 = jnp.int32
    dma = pltpu.SemaphoreType.DMA

    def vmem(shape, kind=f32):
        return pltpu.VMEM(shape, kind)

    loaded = (
        positions, velocities, charges, inverse_mass, export_rows, partners, bond_partners, bond_rest, block_offsets,
    )
    constants = (
        halves(dealt), halves(cas), halves(tall), jnp.asarray(along), jnp.asarray(across), jnp.asarray(freq),
    )
    tile = (8, LANES)
    patches = tiles * pens
    scratch = [vmem(x.shape, x.dtype) for x in loaded]
    scratch[5:8] = [
        vmem((subs, slots, atoms), i32), vmem((subs, bond_rows, atoms), i32), vmem((subs, bond_rows, atoms)),
    ]
    kernel = functools.partial(
        program_kernel, tiles=tiles, pens=pens, subs=subs, planes=planes, deep=deep, share=share, lows=lows,
        chunk=chunk, keep=keep,
    )
    out = pl.pallas_call(
        kernel,
        out_shape=jax.ShapeDtypeStruct((7, 1, atoms), f32),
        in_specs=[hbm] * (len(loaded) + len(constants)),
        out_specs=pl.BlockSpec(memory_space=pltpu.VMEM),
        scratch_shapes=scratch
        + [vmem((2, dealt.shape[1], GRID), bf16)]
        + [vmem(x.shape, x.dtype) for x in constants[1:5]]
        + [
            vmem((share, 2, GRID)),
            vmem((chunks + 1,) + tile), vmem((INNER, 4, LANES)), vmem((INNER, near, 4, LANES)),
            vmem((patches, 4, atoms)), vmem((patches, 4, atoms)), vmem((4, atoms)),
            vmem((chunks + 1, groups) + tile, i32), vmem((chunks + 1, groups) + tile, i32),
            vmem((chunks + 1, groups) + tile), vmem((chunks + 1, groups) + tile), vmem((chunks + 1, groups) + tile),
            vmem((chunks + 1, groups, 3) + tile), vmem((chunks + 1, 3) + tile),
            vmem((chunks + 1, bond_tiles) + tile, i32), vmem((chunks + 1, bond_tiles) + tile),
            vmem((share, GRID + 8, GRID)), vmem((tiles, deep, wide_atoms)), vmem((tiles, share, wide_atoms)),
            vmem((share, wide_atoms)), vmem((tiles if keep else 1, 2, GRID, wide_atoms), bf16),
            vmem((tiles, 4 * GRID, wide_atoms) if keep else (1, 8, LANES)),
            vmem((tiles, 4 * share, wide_atoms) if keep else (1, 8, LANES)),
            vmem((group, 1, width)), vmem((group, 1, width)),
            dma((15,)), dma((INNER, near)), dma((INNER, near)), dma((4, subs)), dma((4, subs)),
            dma((patches,)), dma((patches,)), dma((group,)), dma((patches,)), dma((group,)), dma((group,)),
        ],
        compiler_params=pltpu.CompilerParams(
            collective_id=0, has_side_effects=True, vmem_limit_bytes=VMEM_LIMIT
        ),
    )(*loaded, *constants)
    return out[0:3].reshape(positions.shape), out[3:6].reshape(velocities.shape), out[6:7, :, :width]


def solution(mesh):
    placed = (
        P("rep", "tile", "pen", None),
        P("rep", "tile", "pen", None),
        P(("rep", "tile"), "pen", None),
        P(("rep", "tile"), "pen", None),
        P(("rep", "tile"), "pen", None),
        P(("rep", "tile"), "pen", "sub", None),
        P(("rep", "tile"), "pen", "sub", None),
        P(("rep", "tile"), "pen", "sub", None),
        P("rep", "tile", "pen", None),
    )
    return jax.shard_map(
        on_device,
        mesh=mesh,
        in_specs=placed,
        out_specs=(
            P("rep", "tile", "pen", None),
            P("rep", "tile", "pen", None),
            P(("rep", "tile"), "pen", "sub"),
        ),
        check_vma=False,
    )
```

```python
import functools
import math

import jax
import jax.numpy as jnp
import numpy as np
from jax import lax
from jax.experimental import pallas as pl
from jax.experimental.pallas import tpu as pltpu
from jax.sharding import PartitionSpec as P

GRID = 256
INNER = 4
LANES = 128
LOW = 128
BATCH = 8
VMEM_LIMIT = 60 * 1024 * 1024

time_step = 0.1
coulomb = 30.0
bond_stiffness = 0.2
soften = 1.0
cutoff_sq = 144.0
ewald_beta = 0.32

f32 = jnp.float32
bf16 = jnp.bfloat16


def lane_gather(rows, low):
    return jnp.take_along_axis(rows, low, axis=1, mode="promise_in_bounds")


def split(value):
    high = value.astype(bf16)
    return high, (value - high.astype(f32)).astype(bf16)


def single(left, right, turned=False):
    dims = (((1,), (1 if turned else 0,)), ((), ()))
    return lax.dot_general(left, right, dims, preferred_element_type=f32)


def product(left, right, turned=False):
    return single(left[0], right[0], turned) + (
        single(left[0], right[1], turned) + single(left[1], right[0], turned)
    )


def half_product(left, right, turned=False):
    return single(left[0], right, turned) + single(left[1], right, turned)


def spline_pieces(frac):
    rest = 1.0 - frac
    square = frac * frac
    cube = square * frac
    sixth = 1.0 / 6.0
    return (
        rest * rest * rest * sixth,
        (3.0 * cube - 6.0 * square + 4.0) * sixth,
        (-3.0 * cube + 3.0 * square + 3.0 * frac + 1.0) * sixth,
        cube * sixth,
    )


def spline(place, frac):
    pieces = spline_pieces(frac)
    total = jnp.zeros(place.shape, f32)
    for order in range(4):
        total = jnp.where(place == order, pieces[order], total)
    return total


def wide_row(row):
    return jnp.broadcast_to(row, (8, LANES))


def stacked(rows):
    place = lax.broadcasted_iota(jnp.int32, (8, LANES), 0)
    total = jnp.zeros((8, LANES), rows[0].dtype)
    for r, row in enumerate(rows):
        total = jnp.where(place == r, wide_row(row), total)
    return total


def program_kernel(
    pos_hbm, vel_hbm, chg_hbm, imass_hbm, shown_hbm, parts_hbm, bonds_hbm, rest_hbm, offs_hbm,
    mine_hbm, cas_hbm, tall_hbm, along_hbm, across_hbm, freq_hbm,
    out_ref,
    pos_in, vel_in, chg_in, imass_in, shown_in, parts_all, bonds_all, rest_all, offs_in,
    mine_ref, cas_ref, tall_ref, along_ref, across_ref, freq_ref,
    mine, sent, beside, static_all, pos_all, speeds,
    low_ref, blk_ref, shx_ref, shy_ref, qq_ref, near_ref, bforce, bidx_ref, brest_ref,
    grid, wx, wy, wyq, wz, gz, gy, infl_ref, part_sent, part_recv,
    load_sem, step_send, step_recv, pair_send, pair_recv,
    static_send, static_recv, place_send, place_recv, part_send_sem, part_recv_sem,
    *, tiles, pens, subs, planes, deep, share, lows, chunk, keep,
):
    ti, pi, si = lax.axis_index("tile"), lax.axis_index("pen"), lax.axis_index("sub")
    lead = subs - 1
    leads = si == lead
    local = pens * subs
    group = tiles * local
    patch = ti * pens + pi
    me = patch * subs + si
    atoms = pos_in.shape[3]
    width = atoms // subs
    chunks = atoms // LANES
    shown_chunk = chunks
    slots = parts_all.shape[1]
    groups = subs * slots // 8
    bond_rows = bonds_all.shape[1]
    everyone = range(chunks + 1)

    offsets = []
    for i in range(3):
        for j in range(3):
            step = ((i - 1) % tiles, (j - 1) % pens)
            if step != (0, 0) and step not in offsets:
                offsets.append(step)

    def remote(src, dst, send, recv, device):
        return pltpu.make_async_remote_copy(
            src_ref=src, dst_ref=dst, send_sem=send, recv_sem=recv,
            device_id=device, device_id_type=pl.DeviceIdType.MESH,
        )

    def shifted(index, step, count):
        if isinstance(step, int):
            moved = index + step % count
            return moved if step % count == 0 else jnp.where(moved >= count, moved - count, moved)
        return lax.rem(index + step, count)

    bits = []
    if tiles & (tiles - 1) == 0:
        bits = [lax.rem(lax.div(ti, 1 << b), 2) for b in range(tiles.bit_length() - 1)]

    def tile_at(s):
        if tiles & (tiles - 1):
            return shifted(ti, s, tiles)
        total = ti * 0
        for b, bit in enumerate(bits):
            if isinstance(s, int):
                total = total + ((1 - bit) if (s >> b) & 1 else bit) * (1 << b)
            else:
                total = total + lax.rem(bit + lax.rem(lax.div(s, 1 << b), 2), 2) * (1 << b)
        return total

    def peer(d):
        if isinstance(d, int):
            s, rest = divmod(d, local)
            p, q = divmod(rest, subs)
        else:
            s, rest = lax.div(d, local), lax.rem(d, local)
            p, q = lax.div(rest, subs), lax.rem(rest, subs)
        t, p, q = tile_at(s), shifted(pi, p, pens), shifted(si, q, subs)
        return {"tile": t, "pen": p, "sub": q}, (t * pens + p) * subs + q

    def each(first, last, body):
        if last - first <= 32:
            for d in range(first, last):
                body(d)
        else:
            def step(d, carry):
                body(d)
                return carry

            lax.fori_loop(first, last, step, 0)

    first_loads = [
        (parts_hbm.at[0, 0], parts_all.at[si]), (bonds_hbm.at[0, 0], bonds_all.at[si]),
        (rest_hbm.at[0, 0], rest_all.at[si]),
        (pos_hbm, pos_in), (vel_hbm, vel_in), (chg_hbm, chg_in), (imass_hbm, imass_in),
        (shown_hbm, shown_in), (offs_hbm, offs_in),
    ]
    later_loads = [
        (along_hbm, along_ref), (across_hbm, across_ref), (freq_hbm.at[me], freq_ref),
        (mine_hbm.at[:, me], mine_ref), (cas_hbm, cas_ref), (tall_hbm, tall_ref),
    ]
    loads = [
        pltpu.make_async_copy(src, dst, load_sem.at[k]) for k, (src, dst) in enumerate(first_loads + later_loads)
    ]
    for copy in loads[: len(first_loads)]:
        copy.start()

    barrier = pltpu.get_barrier_semaphore()
    each(
        1, group,
        lambda d: pl.semaphore_signal(
            barrier, inc=1, device_id=peer(d)[0], device_id_type=pl.DeviceIdType.MESH
        ),
    )
    for copy in loads[len(first_loads) :]:
        copy.start()
    for copy in loads[: len(first_loads)]:
        copy.wait()

    shown = jnp.broadcast_to(shown_in[0], (8, LANES))
    shown_low, shown_high = shown & (LANES - 1), shown >> 7

    def show(blocks):
        total = jnp.zeros((8, LANES), blocks[0].dtype)
        for c, block in enumerate(blocks):
            total = jnp.where(shown_high == c, lane_gather(block, shown_low), total)
        return total

    for c in range(chunks):
        lanes = slice(c * LANES, (c + 1) * LANES)
        rows = [pos_in[r, 0, :, lanes] for r in range(3)] + [chg_in[0, :, lanes]]
        rows += [vel_in[r, 0, :, lanes] for r in range(3)] + [imass_in[0, :, lanes]]
        mine[c] = stacked(rows)
        offset = stacked([offs_in[r, 0, :, lanes].astype(f32) for r in range(3)])
        static_all[patch, :, lanes] = offset[:4]
    mine[shown_chunk] = show([mine[c] for c in range(chunks)])

    def step_copy(n, slot):
        dt, dp = offsets[slot]
        back = offsets.index(((-dt) % tiles, (-dp) % pens))
        device = {"tile": shifted(ti, dt, tiles), "pen": shifted(pi, dp, pens)}
        return remote(sent.at[n], beside.at[n, back], step_send.at[n, slot], step_recv.at[n, back], device)

    def send_shown(n):
        sent[n] = mine[shown_chunk][:4]
        for slot in reversed(range(len(offsets))):
            step_copy(n, slot).start()

    def wait_shown(n):
        for slot in range(len(offsets)):
            remote(
                sent.at[n], beside.at[n, slot], step_send.at[n, slot], step_recv.at[n, slot], {"sub": si}
            ).wait_recv()
            step_copy(n, slot).wait_send()

    def pair_copy(k, source):
        table = (parts_all, bonds_all, rest_all, speeds)[k]
        if k == 3:
            return remote(speeds, speeds, pair_send.at[k, source], pair_recv.at[k, lead], {"sub": source})
        return remote(table.at[source], table.at[source], pair_send.at[k, source], pair_recv.at[k, source], {"sub": lead})

    def static_device(d):
        return {"tile": tile_at(d // pens if isinstance(d, int) else lax.div(d, pens)),
                "pen": shifted(pi, d % pens if isinstance(d, int) else lax.rem(d, pens), pens)}

    def static_copy(d):
        return remote(
            static_all.at[patch], static_all.at[patch], static_send.at[d], static_recv.at[patch], static_device(d)
        )

    moves_x, moves_y = [], []
    for i in range(3):
        near = ti + (i - 1)
        moves_x.append(jnp.where(near < 0, -float(GRID), jnp.where(near >= tiles, float(GRID), 0.0)))
        near = pi + (i - 1)
        moves_y.append(jnp.where(near < 0, -float(GRID), jnp.where(near >= pens, float(GRID), 0.0)))

    def work_out(c, g, index):
        high = index >> 7
        block = high
        shx = jnp.zeros((8, LANES), f32)
        shy = jnp.zeros((8, LANES), f32)
        for i in range(3):
            for j in range(3):
                if (i, j) == (1, 1):
                    continue
                hit = high == chunks + i * 3 + j
                step = ((i - 1) % tiles, (j - 1) % pens)
                block = jnp.where(hit, chunks + offsets.index(step), block)
                if i != 1:
                    shx = jnp.where(hit, moves_x[i], shx)
                if j != 1:
                    shy = jnp.where(hit, moves_y[j], shy)
        low_ref[c, g] = index & (LANES - 1)
        blk_ref[c, g] = block
        shx_ref[c, g] = shx
        shy_ref[c, g] = shy

    def set_up_rows(some):
        for g in range(groups):
            q, row = divmod(g * 8, slots)
            if q not in some:
                continue
            index = [parts_all[q, row : row + 8, c * LANES : (c + 1) * LANES] for c in range(chunks)]
            for c in everyone:
                work_out(c, g, show(index) if c == shown_chunk else index[c])

    def set_up():
        for source in range(lead):
            for k in range(3):
                pair_copy(k, source).wait_recv()
        set_up_rows(range(lead))
        rows_of = [(q, b) for q in range(subs) for b in range(bond_rows)]
        for v in range(bidx_ref.shape[1]):
            part = rows_of[v * 8 : v * 8 + 8]
            numbers, rests = [], []
            for c in range(chunks):
                lanes = slice(c * LANES, (c + 1) * LANES)
                atom = lax.broadcasted_iota(jnp.int32, (1, LANES), 1) + c * LANES
                rows = [bonds_all[q, b : b + 1, lanes] for q, b in part] + [atom] * (8 - len(part))
                numbers.append(stacked(rows))
                rests.append(stacked([rest_all[q, b : b + 1, lanes] for q, b in part]))
                bidx_ref[c, v] = numbers[c]
                brest_ref[c, v] = rests[c]
            bidx_ref[shown_chunk, v] = show(numbers)
            brest_ref[shown_chunk, v] = show(rests)

    def own_tables(rows):
        return [(c, [wide_row(mine[c, r : r + 1, :]) for r in rows]) for c in range(chunks)]

    def around_tables(n, rows):
        return [
            (chunks + slot, [wide_row(beside[n, slot, r : r + 1, :]) for r in rows]) for slot in range(len(offsets))
        ]

    def pick(found, low, block, table):
        for number, sources in table:
            hit = block == number
            found = [jnp.where(hit, lane_gather(source, low), f) for source, f in zip(sources, found)]
        return found

    xyz = (0, 1, 2)

    def near_part():
        table = own_tables(xyz)
        for c in everyone:
            for g in range(groups):
                found = pick([jnp.zeros((8, LANES), f32)] * 3, low_ref[c, g], blk_ref[c, g], table)
                near_ref[c, g, 0] = found[0] + shx_ref[c, g]
                near_ref[c, g, 1] = found[1] + shy_ref[c, g]
                near_ref[c, g, 2] = found[2]
            own = [wide_row(mine[c, r : r + 1, :]) for r in xyz]
            force = [jnp.zeros((8, LANES), f32)] * 3
            for v in range(bidx_ref.shape[1]):
                index = bidx_ref[c, v]
                near = pick([jnp.zeros((8, LANES), f32)] * 3, index & (LANES - 1), index >> 7, table)
                delta = [own[r] - near[r] for r in xyz]
                root = lax.rsqrt(delta[0] * delta[0] + delta[1] * delta[1] + delta[2] * delta[2] + soften)
                pull = -bond_stiffness * (1.0 - brest_ref[c, v] * root)
                force = [force[r] + pull * delta[r] for r in xyz]
            for r in xyz:
                bforce[c, r] = force[r]

    def far_part(n, which):
        table = around_tables(n, xyz)
        for c in which:
            own = [wide_row(mine[c, r : r + 1, :]) for r in xyz]
            force = [bforce[c, r] for r in xyz]
            for g in range(groups):
                shift = (shx_ref[c, g], shy_ref[c, g], 0.0)
                near = [near_ref[c, g, r] for r in xyz]
                low, block = low_ref[c, g], blk_ref[c, g]
                inside = block < chunks
                far = pick([jnp.zeros((8, LANES), f32)] * 3, low, block, table)
                near = [
                    jnp.where(inside, near[r], far[r] if r == 2 else far[r] + shift[r]) for r in xyz
                ]
                delta = [own[r] - near[r] for r in xyz]
                dist_sq = delta[0] * delta[0] + delta[1] * delta[1] + delta[2] * delta[2]
                taper = 1.0 - dist_sq * (1.0 / cutoff_sq)
                taper = jnp.where(dist_sq < cutoff_sq, taper * taper, 0.0)
                root = lax.rsqrt(dist_sq + soften)
                strength = qq_ref[c, g] * taper * (root * root * root)
                force = [force[r] + strength * delta[r] for r in xyz]
            scale = mine[c, 7:8, :]
            for r in xyz:
                total = jnp.sum(force[r], axis=0, keepdims=True)
                speed = mine[c, 4 + r : 5 + r, :] + time_step * scale * total
                mine[c, 4 + r : 5 + r, :] = speed
                mine[c, r : r + 1, :] = mine[c, r : r + 1, :] + time_step * speed

    def charges_once():
        table = own_tables((3,)) + around_tables(0, (3,))
        for c in everyone:
            own = wide_row(mine[c, 3:4, :])
            for g in range(groups):
                (near,) = pick([jnp.zeros((8, LANES), f32)], low_ref[c, g], blk_ref[c, g], table)
                qq_ref[c, g] = coulomb * own * near

    wide_atoms = local * width

    def cells(offset, count):
        return lax.broadcasted_iota(jnp.int32, (count, wide_atoms), 0) - offset

    def row_of(ref, t, r):
        return jnp.concatenate([ref[t * pens + p, r : r + 1, :] for p in range(pens)], axis=1)

    def static_wait(q):
        remote(
            static_all.at[patch], static_all.at[q], static_send.at[0], static_recv.at[q], {"sub": si}
        ).wait_recv()

    def place_wait(q):
        remote(
            pos_all.at[patch], pos_all.at[q], place_send.at[0], place_recv.at[q], {"sub": si}
        ).wait_recv()

    def tile_wait(wait, s, t, own_too):
        for step in range(1, pens):
            wait(t * pens + shifted(pi, step, pens))

        @pl.when(jnp.logical_or(s > 0, own_too))
        def _():
            wait(t * pens + pi)

    def fill(s):
        t = tile_at(s)
        tile_wait(static_wait, s, t, False)
        for r, source, target in ((1, mine_ref, gy), (2, cas_ref, gz)):
            offset = (row_of(static_all, t, r).astype(jnp.int32) + 1) & (GRID - 1)
            hot = jnp.where(cells(offset, GRID) == 0, 1.0, 0.0).astype(bf16)
            rows = source.shape[1]
            part = min(rows, GRID)
            for c in range(0, rows, part):
                value = single(source[0, c : c + part], hot) + single(source[1, c : c + part], hot)
                target[t, c : c + part] = value

    def fill_step(n):
        per = -(-tiles // INNER)
        for k in range(per):
            s = n * per + k
            if tiles % INNER:
                pl.when(s < tiles)(functools.partial(fill, s))
            else:
                fill(s)

    pl.when(leads)(functools.partial(set_up_rows, [lead]))
    early = keep and share % INNER == 0

    def influence(k):
        m_sq = along_ref[...] + freq_ref[k, 0:1, :]
        anchor = m_sq == 0.0
        value = across_ref[...] * freq_ref[k, 1:2, :] / jnp.where(anchor, 1.0, m_sq)
        return jnp.where(anchor, 0.0, value)

    ready = loads[len(first_loads) : len(first_loads) + 3]
    for copy in ready:
        copy.wait()
    if early:
        def influence_row(k, carry):
            infl_ref[k] = influence(k)
            return carry

        lax.fori_loop(0, share, influence_row, 0)
    pl.semaphore_wait(barrier, group - 1)

    @pl.when(leads)
    def _():
        send_shown(0)

    for source in range(lead):
        @pl.when(si == source)
        def _(source=source):
            for k in range(3):
                pair_copy(k, source).start()

    each(1, tiles * pens, lambda d: static_copy(d).start())

    @pl.when(leads)
    def _():
        set_up()

    for copy in loads[len(first_loads) + 3 :]:
        copy.wait()

    def clear(j, carry):
        for edge in range(tiles + 1):
            grid[j, edge * planes : edge * planes + 8] = jnp.zeros((8, GRID), f32)
        return carry

    lax.fori_loop(0, share, clear, 0)

    def inner(n, carry):
        @pl.when(leads)
        def _():
            @pl.when(n > 0)
            def _():
                far_part(n - 1, [shown_chunk])
                send_shown(n)
                far_part(n - 1, range(chunks))

            near_part()

        if keep:
            fill_step(n)

        @pl.when(leads)
        def _():
            wait_shown(n)

            @pl.when(n == 0)
            def _():
                charges_once()

        return carry

    lax.fori_loop(0, INNER, inner, 0)

    def place_copy(d):
        return remote(pos_all.at[patch], pos_all.at[patch], place_send.at[d], place_recv.at[patch], peer(d)[0])

    @pl.when(leads)
    def _():
        far_part(INNER - 1, range(chunks))
        for c in range(chunks):
            lanes = slice(c * LANES, (c + 1) * LANES)
            pos_all[patch, :, lanes] = mine[c][:4]
            speeds[:, lanes] = mine[c][4:]
        each(1, group, lambda d: place_copy(d).start())
        for source in range(lead):
            pair_copy(3, source).start()

    if not keep:
        each(1, tiles * pens, lambda d: static_wait(
            static_device(d)["tile"] * pens + static_device(d)["pen"]
        ))
    each(1, tiles * pens, lambda d: static_copy(d).wait_send())
    top = tiles * planes

    def prepare(t, r):
        offset = row_of(static_all, t, r)
        return offset.astype(jnp.int32), row_of(pos_all, t, r) - (offset + 1.0)

    def blend(table, start, count, pieces):
        rows = table.shape[0] // 4
        total = table[start : start + count] * pieces[0]
        for m in range(1, 4):
            total = total + table[m * rows + start : m * rows + start + count] * pieces[m]
        return total

    def depth_of(t):
        offset, frac = prepare(t, 2)
        depth = spline(cells(offset, GRID) & (GRID - 1), frac)
        return split(product((cas_ref[0, GRID : 2 * GRID], cas_ref[1, GRID : 2 * GRID]), split(depth)))

    parts = [(c, min(c + chunk, lows), True) for c in range(0, lows, chunk)]
    parts += [(c, min(c + chunk, share), False) for c in range(lows, share, chunk)]

    def spread(s, carry):
        t = tile_at(s)
        tile_wait(place_wait, s, t, jnp.logical_not(leads))
        offset, frac = prepare(t, 0)
        wx[t] = spline(cells(offset - (t * planes - 1), deep), frac)
        offset, frac = prepare(t, 1)
        if keep:
            wy[t] = blend(gy.at[t], 0, share, spline_pieces(frac))
            pieces = spline_pieces(prepare(t, 2)[1])
            for c in range(0, GRID, 64):
                high, low = split(blend(gz.at[t], c, 64, pieces))
                wz[t, 0, c : c + 64] = high
                wz[t, 1, c : c + 64] = low
            depth = (wz[t, 0], wz[t, 1])
        else:
            rows = spline(cells(offset, GRID) & (GRID - 1), frac)
            wy[t] = product((mine_ref[0, share : 2 * share], mine_ref[1, share : 2 * share]), split(rows))
            depth = depth_of(t)
        wyq[...] = wy[t] * row_of(pos_all, t, 3)
        base = pl.multiple_of(t * planes, 8)
        for start, stop, exact in parts:
            plane = jnp.concatenate([wx[t] * wyq[k : k + 1, :] for k in range(start, stop)], axis=0)
            if exact:
                values = product(split(plane), depth, True)
            else:
                values = single(plane.astype(bf16), depth[0], True)
            values = values.reshape(stop - start, deep, GRID)
            for k in range(start, stop):
                value = values[k - start]
                grid[k, pl.ds(base, 8)] += value[:8]
                if planes > 8:
                    grid[k, pl.ds(pl.multiple_of(base + 8, 8), planes - 8)] = value[8:planes]
                grid[k, pl.ds(pl.multiple_of(base + planes, 8), 8)] += value[planes : planes + 8]
        return carry

    lax.fori_loop(0, tiles, spread, 0)
    for source in range(lead):
        @pl.when(si == source)
        def _(source=source):
            remote(
                speeds, speeds, pair_send.at[3, source], pair_recv.at[3, lead], {"sub": lead}
            ).wait_recv()
    for r in range(3):
        out_ref[r] = pos_all[patch, r : r + 1, :]
        out_ref[3 + r] = speeds[r : r + 1, :]

    def transform(start, stop, exact):
        batch = math.gcd(math.gcd(start, stop), BATCH)

        def step(n, carry):
            first = start + n * batch
            lines = []
            for i in range(batch):
                line = grid[first + i, 0:top]
                edge = line[:8] + grid[first + i, top : top + 8]
                lines.append(jnp.concatenate([edge, line[8:]], axis=0))
            line = split(jnp.concatenate(lines, axis=1))
            spectrum = product((cas_ref[0, :GRID], cas_ref[1, :GRID]), line)
            weighted = []
            for i in range(batch):
                value = infl_ref[first + i] if early else influence(first + i)
                weighted.append(spectrum[:, i * GRID : (i + 1) * GRID] * value)
            weighted = jnp.concatenate(weighted, axis=1)
            if exact:
                back = product((tall_ref[0], tall_ref[1]), split(weighted))
            else:
                back = half_product((tall_ref[0], tall_ref[1]), weighted.astype(bf16))
            for i in range(batch):
                grid[first + i, 0:top] = back[:, i * GRID : (i + 1) * GRID]
                grid[first + i, top : top + 8] = back[0:8, i * GRID : (i + 1) * GRID]
            return carry

        if stop > start:
            lax.fori_loop(0, (stop - start) // batch, step, 0)

    transform(0, lows, True)
    transform(lows, share, False)

    def part_copy(g, device):
        return remote(part_sent.at[g], part_recv.at[me], part_send_sem.at[g], part_recv_sem.at[me], device)

    def read(n, carry):
        s = tiles - 1 - n
        t = tile_at(s)
        if keep:
            depth = (wz[t, 0], wz[t, 1])
        else:
            depth = depth_of(t)
        base = pl.multiple_of(t * planes, 8)
        total = jnp.zeros((planes + 8, wide_atoms), f32)
        for start, stop, exact in parts:
            rows = [grid[k, pl.ds(base, planes + 8)] for k in range(start, stop)]
            line = jnp.concatenate(rows, axis=0)
            if exact:
                values = product(split(line), depth)
            else:
                values = single(line.astype(bf16), depth[0])
            for k in range(start, stop):
                part = values[(k - start) * (planes + 8) : (k - start + 1) * (planes + 8)]
                total = total + part * wy[t, k : k + 1, :]
        result = jnp.sum(total * wx[t, : planes + 8], axis=0, keepdims=True)
        for q in range(local):
            part_sent[t * local + q] = result[:, q * width : (q + 1) * width]

        def give(p, q):
            device = {"tile": t, "pen": p, "sub": q}
            part_copy((t * pens + p) * subs + q, device).start()

        for d in range(1, local):
            give(shifted(pi, d // subs, pens), shifted(si, d % subs, subs))

        @pl.when(s > 0)
        def _():
            give(pi, si)

        return carry

    lax.fori_loop(0, tiles, read, 0)
    part_recv[me] = part_sent[me]

    @pl.when(leads)
    def _():
        each(1, group, lambda d: place_copy(d).wait_send())
        for source in range(lead):
            pair_copy(3, source).wait_send()

    for source in range(lead):
        @pl.when(si == source)
        def _(source=source):
            for k in range(3):
                pair_copy(k, source).wait_send()

    def finish(d):
        device, g = peer(d)
        part_copy(g, device).wait_send()
        remote(part_sent.at[me], part_recv.at[g], part_send_sem.at[g], part_recv_sem.at[g], {"sub": si}).wait_recv()

    each(1, group, finish)
    out_ref[6, :, 0:width] = jnp.sum(part_recv[...], axis=0)
    out_ref[6, :, width:] = jnp.zeros((1, atoms - width), f32)


def halves(table):
    table = jnp.asarray(table.astype(np.float32))
    return jnp.stack(split(table))


def tables(group, shifts):
    share = GRID // group
    index = np.arange(GRID)
    angle = 2.0 * math.pi / GRID * np.mod(index[:, None] * index[None, :], GRID)
    cas = np.cos(angle) + np.sin(angle)
    order = np.array([(r + 1) // 2 if r % 2 else (GRID - r // 2) % GRID for r in range(GRID)])
    dealt = order.reshape(share, group).T
    signed = np.where(index > GRID // 2, index - GRID, index).astype(np.float64)
    turn = 2.0 * math.pi / GRID * index
    real = (1.0 + 4.0 * np.cos(turn) + np.cos(2.0 * turn)) / 6.0
    imag = (4.0 * np.sin(turn) + np.sin(2.0 * turn)) / 6.0
    square = signed**2 / float(GRID * GRID)
    line = np.exp(-((math.pi / ewald_beta) ** 2) * square) / (real * real + imag * imag)
    along = square[:, None] + 0.5 * square[None, :]
    across = line[:, None] * np.sqrt(line)[None, :] / (math.pi * float(GRID) ** 3)
    freq = np.stack(
        [square[dealt][..., None] + 0.5 * square, line[dealt][..., None] * np.sqrt(line)], axis=2
    )
    shifted = [cas[:, np.mod(index + m, GRID)] for m in range(-1, shifts - 1)]
    return (
        np.concatenate(shifted), shifted[0].T, np.concatenate([cells[dealt] for cells in shifted], axis=1),
        freq.astype(np.float32), along.astype(np.float32), across.astype(np.float32),
    )


def on_device(
    positions, velocities, charges, inverse_mass, export_rows, partners, bond_partners, bond_rest, block_offsets,
):
    tiles, pens, subs = lax.axis_size("tile"), lax.axis_size("pen"), lax.axis_size("sub")
    local = pens * subs
    group = tiles * local
    atoms, exported = positions.shape[3], export_rows.shape[2]
    slots, bond_rows = partners.shape[2], bond_partners.shape[2]
    width = atoms // subs
    chunks = atoms // LANES
    groups = subs * slots // 8
    planes = GRID // tiles
    share = GRID // group
    lows = min(share, max(1, -(-LOW // group)))
    chunk = math.gcd(share, 8)
    unit = 8 if chunk % 2 == 0 else 16
    deep = -(-(planes + 8) // unit) * unit
    wide_atoms = local * width
    keep = group * width * GRID * 4 <= 16 * 1024 * 1024
    cas, tall, dealt, freq, along, across = tables(group, 4 if keep else 2)
    around = {((i - 1) % tiles, (j - 1) % pens) for i in range(3) for j in range(3)} - {(0, 0)}
    near = len(around)
    bond_tiles = -(-subs * bond_rows // 8)
    assert exported == LANES and slots % 8 == 0 and planes % 8 == 0
    hbm = pl.BlockSpec(memory_space=pltpu.HBM)
    i32 = jnp.int32
    dma = pltpu.SemaphoreType.DMA

    def vmem(shape, kind=f32):
        return pltpu.VMEM(shape, kind)

    loaded = (
        positions, velocities, charges, inverse_mass, export_rows, partners, bond_partners, bond_rest, block_offsets,
    )
    constants = (
        halves(dealt), halves(cas), halves(tall), jnp.asarray(along), jnp.asarray(across), jnp.asarray(freq),
    )
    tile = (8, LANES)
    patches = tiles * pens
    scratch = [vmem(x.shape, x.dtype) for x in loaded]
    scratch[5:8] = [
        vmem((subs, slots, atoms), i32), vmem((subs, bond_rows, atoms), i32), vmem((subs, bond_rows, atoms)),
    ]
    kernel = functools.partial(
        program_kernel, tiles=tiles, pens=pens, subs=subs, planes=planes, deep=deep, share=share, lows=lows,
        chunk=chunk, keep=keep,
    )
    out = pl.pallas_call(
        kernel,
        out_shape=jax.ShapeDtypeStruct((7, 1, atoms), f32),
        in_specs=[hbm] * (len(loaded) + len(constants)),
        out_specs=pl.BlockSpec(memory_space=pltpu.VMEM),
        scratch_shapes=scratch
        + [vmem((2, dealt.shape[1], GRID), bf16)]
        + [vmem(x.shape, x.dtype) for x in constants[1:5]]
        + [
            vmem((share, 2, GRID)),
            vmem((chunks + 1,) + tile), vmem((INNER, 4, LANES)), vmem((INNER, near, 4, LANES)),
            vmem((patches, 4, atoms)), vmem((patches, 4, atoms)), vmem((4, atoms)),
            vmem((chunks + 1, groups) + tile, i32), vmem((chunks + 1, groups) + tile, i32),
            vmem((chunks + 1, groups) + tile), vmem((chunks + 1, groups) + tile), vmem((chunks + 1, groups) + tile),
            vmem((chunks + 1, groups, 3) + tile), vmem((chunks + 1, 3) + tile),
            vmem((chunks + 1, bond_tiles) + tile, i32), vmem((chunks + 1, bond_tiles) + tile),
            vmem((share, GRID + 8, GRID)), vmem((tiles, deep, wide_atoms)), vmem((tiles, share, wide_atoms)),
            vmem((share, wide_atoms)), vmem((tiles if keep else 1, 2, GRID, wide_atoms), bf16),
            vmem((tiles, 4 * GRID, wide_atoms) if keep else (1, 8, LANES)),
            vmem((tiles, 4 * share, wide_atoms) if keep else (1, 8, LANES)),
            vmem((share, GRID, GRID) if keep and share % INNER == 0 else (1, 8, LANES)),
            vmem((group, 1, width)), vmem((group, 1, width)),
            dma((15,)), dma((INNER, near)), dma((INNER, near)), dma((4, subs)), dma((4, subs)),
            dma((patches,)), dma((patches,)), dma((group,)), dma((patches,)), dma((group,)), dma((group,)),
        ],
        compiler_params=pltpu.CompilerParams(
            collective_id=0, has_side_effects=True, vmem_limit_bytes=VMEM_LIMIT
        ),
    )(*loaded, *constants)
    return out[0:3].reshape(positions.shape), out[3:6].reshape(velocities.shape), out[6:7, :, :width]


def solution(mesh):
    placed = (
        P("rep", "tile", "pen", None),
        P("rep", "tile", "pen", None),
        P(("rep", "tile"), "pen", None),
        P(("rep", "tile"), "pen", None),
        P(("rep", "tile"), "pen", None),
        P(("rep", "tile"), "pen", "sub", None),
        P(("rep", "tile"), "pen", "sub", None),
        P(("rep", "tile"), "pen", "sub", None),
        P("rep", "tile", "pen", None),
    )
    return jax.shard_map(
        on_device,
        mesh=mesh,
        in_specs=placed,
        out_specs=(
            P("rep", "tile", "pen", None),
            P("rep", "tile", "pen", None),
            P(("rep", "tile"), "pen", "sub"),
        ),
        check_vma=False,
    )
```
